256 devices in a mesh: vpair: 16 (over x, y), rank: 16 (over z, core).
Axes of the slice: x: 4, y: 4, z: 8, core: 2. Of those that a mesh axis runs over, the one named last changes fastest.
Arguments:
- amplitudes: bfloat16 [8, 1200, 1200], P(None, 'vpair', 'rank'), may hold values from -6 to 6
- factors: bfloat16 [1200, 8192], P('vpair', 'rank'), may hold values from -0.1875 to 0.1875
- kernel: bfloat16 [8192, 8192], P('vpair', 'rank'), may hold values from -0.875 to 0.875
- other_terms: float32 [8, 1200, 1200], P(None, 'vpair'), may hold values from -6 to 6
- virt_energy: float32 [1200], replicated, may hold values from 0.2 to 4
- pair_energy: float32 [8], replicated, may hold values from -3 to -0.5
Outputs:
- residual: float32 [8, 1200, 1200], P(None, 'vpair')
- update_rms: float32 [], replicated
The draws below stay inside these ranges and needn't reach their ends.
All inputs are finite; a program needn't handle non-finite values.
Results may differ from the reference program's by a relative error of at most 0.0035.
Values may be sent and summed in bfloat16 or wider, within the bound.
No kernel may reach another device: no remote copies, remote signals or barrier semaphores. Data moves between devices by JAX's collectives and lax.ppermute only.
A program may use at most 192 MiB of HBM per device.

```python
import jax
import jax.numpy as jnp
from jax import lax

NVIR = 1200
NTHC = 8192
PAIRS = 8


def draw_virt_energy(key, part):
    jitter = jax.random.uniform(key, (NVIR,), jnp.float32)
    spread = (jnp.arange(NVIR, dtype=jnp.float32) + jitter) / NVIR
    return 0.2 + 3.8 * spread


def block_levels(rng, dims, split, smallest, largest):
    gain = 1.0
    for axis_at, parts in split:
        heights = jax.random.uniform(jax.random.fold_in(jax.random.fold_in(rng, 6), axis_at), (parts,), jnp.float32, smallest / len(split), largest / len(split))
        gain = gain * jnp.repeat(jnp.exp(heights), dims[axis_at] // parts).reshape((-1,) + (1,) * (len(dims) - 1 - axis_at))
    return gain


def centred(rng, shape, scale, limit, cuts=(), held_as=jnp.bfloat16):
    drawn = scale * jax.random.normal(rng, shape, jnp.float32)
    if cuts:
        drawn = drawn * block_levels(rng, shape, cuts, -0.22, 0.18)
    return jnp.clip(drawn, -limit, limit).astype(held_as)


def setup_inputs(seed: int = 0) -> dict:
    keys = jax.random.split(jax.random.key(seed), 7)
    amplitudes = centred(keys[0], (PAIRS, NVIR, NVIR), 1.0, 6.0, ((1, 16), (2, 16)))
    factors = centred(keys[1], (NVIR, NTHC), NVIR ** -0.5, 0.1875, ((0, 16), (1, 16)))
    kernel = centred(keys[2], (NTHC, NTHC), (NTHC * NTHC // (NVIR * NVIR)) ** -0.5, 0.875, ((0, 16), (1, 16)))
    other_terms = centred(keys[3], (PAIRS, NVIR, NVIR), 1.0, 6.0, ((1, 16),), jnp.float32)
    virt_energy = draw_virt_energy(jax.random.fold_in(keys[6], 71), 0)
    pair_energy = jnp.clip(jax.random.uniform(keys[5], (PAIRS,), jnp.float32, -3.0, -0.5), -3.0, -0.5)
    return dict(amplitudes=amplitudes, factors=factors, kernel=kernel, other_terms=other_terms, virt_energy=virt_energy, pair_energy=pair_energy)


epsilon = 1e-06

def reference(amplitudes, factors, kernel, other_terms, virt_energy, pair_energy):
    kernel_wide = kernel.astype(jnp.float32)

    def one_pair(operands):
        amplitude, other_block, pair_value = operands
        first_half = jnp.dot(amplitude, factors, preferred_element_type=jnp.float32).astype(jnp.bfloat16)
        coupled = jnp.dot(factors.T, first_half, preferred_element_type=jnp.float32)
        weighted = (kernel_wide * coupled).astype(jnp.bfloat16)
        back_half = jnp.dot(factors, weighted, preferred_element_type=jnp.float32).astype(jnp.bfloat16)
        ladder = jnp.dot(back_half, factors.T, preferred_element_type=jnp.float32)
        residual = other_block + ladder
        denominator = virt_energy[:, None] + virt_energy[None, :] - pair_value
        update = residual / denominator
        return (residual, jnp.sum(update * update))
    residual, squares = lax.map(one_pair, (amplitudes, other_terms, pair_energy))
    update_rms = jnp.sqrt(jnp.sum(squares) / (PAIRS * NVIR * NVIR) + epsilon)
    return (residual, update_rms)
```

```python
import jax
import jax.numpy as jnp
from jax import lax
from jax.experimental import pallas as pl
from jax.experimental.pallas import tpu as pltpu
from jax.sharding import Mesh
from jax.sharding import PartitionSpec as P

AXES = ("x", "y", "z", "c")
XY = ("x", "y")
RANK = ("z", "c")
BF = jnp.bfloat16
F32 = jnp.float32
epsilon = 1e-06

NX, NY, NZ, NC = 4, 4, 8, 2
NV = NX * NY
PAIRS = 8
ROW = 75
PAD = 80
BLK = 512
QC = 32
NVIR = 1200
LANE = 128


def core_swap(value):
    return lax.ppermute(value, "c", [(0, 1), (1, 0)])


def regroup(tiles, want):
    out = None
    lane = lax.broadcasted_iota(jnp.int32, (PAD, LANE), 1) // QC
    for group, tile in enumerate(tiles):
        shift = ((group - want) * QC) % LANE
        moved = pltpu.roll(tile, shift, 1) if shift else tile
        out = moved if out is None else jnp.where(lane == group, moved, out)
    return out


def half_kernel(core_ref, own_ref, oth_ref, xq_ref, out_ref, acc_ref):
    core = core_ref[0]
    dims = (((0,), (0,)), ((), ()))
    x_own = xq_ref[:, core].reshape(NZ * PAD, BLK)
    x_oth = xq_ref[:, 1 - core].reshape(NZ * PAD, BLK)
    acc_ref[...] = lax.dot_general(
        own_ref[...], x_own, dims, preferred_element_type=F32
    ) + lax.dot_general(oth_ref[...], x_oth, dims, preferred_element_type=F32)
    for xx in range(NX):
        for half in range(2):
            tiles = [
                acc_ref[pl.ds((half * 4 + g) * PAD, PAD), pl.ds(xx * LANE, LANE)]
                for g in range(4)
            ]
            for yy in range(NY):
                out_ref[xx * NY + yy, :, pl.ds(half * LANE, LANE)] = regroup(tiles, yy).astype(BF)


def make_half(core, t_own, t_oth, xq):
    return pl.pallas_call(
        half_kernel,
        out_shape=jax.ShapeDtypeStruct((NV, PAD, PAIRS * QC), BF),
        in_specs=[pl.BlockSpec(memory_space=pltpu.SMEM)]
        + [pl.BlockSpec(memory_space=pltpu.VMEM)] * 3,
        scratch_shapes=[pltpu.VMEM((PAIRS * PAD, BLK), F32)],
        name="half",
    )(core, t_own, t_oth, xq)


def main_kernel(core_ref, ho_ref, hx_ref, x_ref, zo_ref, zx_ref, bo_ref, bx_ref, h_ref, acc_ref):
    step = pl.program_id(0)
    half_m = PAIRS * QC

    @pl.when(step == 0)
    def _():
        h_ref[pl.ds(0, half_m), :] = ho_ref[...].astype(F32).T.astype(BF)
        h_ref[pl.ds(half_m, half_m), :] = hx_ref[...].astype(F32).T.astype(BF)
        acc_ref[...] = jnp.zeros_like(acc_ref)

    x = x_ref[...].reshape(NV * PAD, BLK)
    coupled = jnp.dot(h_ref[...], x, preferred_element_type=F32)
    z_own = zo_ref[...].reshape(1, QC, BLK).astype(F32)
    z_oth = zx_ref[...].reshape(1, QC, BLK).astype(F32)
    c_own = coupled[:half_m].reshape(PAIRS, QC, BLK) * z_own
    c_oth = coupled[half_m:].reshape(PAIRS, QC, BLK) * z_oth
    w = jnp.concatenate(
        [c_own.reshape(half_m, BLK), c_oth.reshape(half_m, BLK)], axis=0
    ).astype(BF)
    acc_ref[...] += lax.dot_general(x, w, (((1,), (1,)), ((), ())), preferred_element_type=F32)

    @pl.when(step == NZ - 1)
    def _():
        bo_ref[...] = acc_ref[:, :half_m]
        bx_ref[...] = acc_ref[:, half_m:].astype(BF)


def make_main(core, h_own, h_oth, x_all, z_own, z_oth):
    rows = NV * PAD
    half_m = PAIRS * QC
    return pl.pallas_call(
        main_kernel,
        out_shape=(
            jax.ShapeDtypeStruct((rows, half_m), F32),
            jax.ShapeDtypeStruct((rows, half_m), BF),
        ),
        grid_spec=pltpu.PrefetchScalarGridSpec(
            num_scalar_prefetch=1,
            grid=(NZ,),
            in_specs=[
                pl.BlockSpec((rows, half_m), lambda k, c: (0, 0)),
                pl.BlockSpec((rows, half_m), lambda k, c: (0, 0)),
                pl.BlockSpec((NV, 1, PAD, BLK), lambda k, c: (0, k, 0, 0)),
                pl.BlockSpec((1, 1, QC, BLK), lambda k, c: (k, c[0], 0, 0)),
                pl.BlockSpec((1, QC, BLK), lambda k, c: (k, 0, 0)),
            ],
            out_specs=(
                pl.BlockSpec((rows, half_m), lambda k, c: (0, 0)),
                pl.BlockSpec((rows, half_m), lambda k, c: (0, 0)),
            ),
            scratch_shapes=[
                pltpu.VMEM((2 * half_m, rows), BF),
                pltpu.VMEM((rows, 2 * half_m), F32),
            ],
        ),
        compiler_params=pltpu.CompilerParams(dimension_semantics=("arbitrary",)),
        cost_estimate=pl.CostEstimate(
            flops=4 * 512 * 1280 * 4096, bytes_accessed=14_000_000, transcendentals=0
        ),
        name="ladder_core",
    )(core, h_own, h_oth, x_all, z_own, z_oth)


def ladder_kernel(core_ref, b_ref, x_ref, own_ref, oth_ref, g_ref):
    core = core_ref[0]
    for xx in range(NX):
        for half in range(2):
            tiles = [
                b_ref[xx * NY + yy, :, pl.ds(half * LANE, LANE)].astype(F32) for yy in range(NY)
            ]
            for g in range(4):
                g_ref[half, pl.ds(g * PAD, PAD), pl.ds(xx * LANE, LANE)] = regroup(
                    tiles, g
                ).astype(BF)
    dims = (((1,), (1,)), ((), ()))
    own_ref[...] = lax.dot_general(g_ref[core], x_ref[...], dims, preferred_element_type=F32)
    oth_ref[...] = lax.dot_general(
        g_ref[1 - core], x_ref[...], dims, preferred_element_type=F32
    ).astype(BF)


def make_ladder(core, b_all, x_rows):
    return pl.pallas_call(
        ladder_kernel,
        out_shape=(
            jax.ShapeDtypeStruct((4 * PAD, NVIR), F32),
            jax.ShapeDtypeStruct((4 * PAD, NVIR), BF),
        ),
        in_specs=[pl.BlockSpec(memory_space=pltpu.SMEM)]
        + [pl.BlockSpec(memory_space=pltpu.VMEM)] * 2,
        scratch_shapes=[pltpu.VMEM((2, 4 * PAD, BLK), BF)],
        name="ladder_rank",
    )(core, b_all, x_rows)


def final_kernel(core_ref, pair_ref, own_ref, oth_ref, other_ref, row_ref, col_ref, out_ref, sq_ref):
    i = pl.program_id(0)
    mine = (i // 4) == core_ref[0]
    own = own_ref[0, :ROW, :].astype(F32)
    oth = oth_ref[0, :ROW, :].astype(F32)
    res = other_ref[0] + jnp.where(mine, own, oth)
    out_ref[0] = res
    upd = res / (row_ref[...] + col_ref[...] - pair_ref[i])
    part = jnp.sum(upd * upd, axis=0, keepdims=True)

    @pl.when(i == 0)
    def _():
        sq_ref[...] = jnp.zeros_like(sq_ref)

    sq_ref[...] += part


def make_final(core, pair_energy, l_own, l_oth, other_terms, row_energy, col_energy):
    def own_index(i, c, p):
        return (jnp.clip(i - 4 * c[0], 0, 3), 0, 0)

    def oth_index(i, c, p):
        return (jnp.clip(i - 4 * (1 - c[0]), 0, 3), 0, 0)

    return pl.pallas_call(
        final_kernel,
        out_shape=(
            jax.ShapeDtypeStruct((PAIRS, ROW, NVIR), F32),
            jax.ShapeDtypeStruct((1, NVIR), F32),
        ),
        grid_spec=pltpu.PrefetchScalarGridSpec(
            num_scalar_prefetch=2,
            grid=(PAIRS,),
            in_specs=[
                pl.BlockSpec((1, PAD, NVIR), own_index),
                pl.BlockSpec((1, PAD, NVIR), oth_index),
                pl.BlockSpec((1, ROW, NVIR), lambda i, c, p: (i, 0, 0)),
                pl.BlockSpec((ROW, 1), lambda i, c, p: (0, 0)),
                pl.BlockSpec((1, NVIR), lambda i, c, p: (0, 0)),
            ],
            out_specs=(
                pl.BlockSpec((1, ROW, NVIR), lambda i, c, p: (i, 0, 0)),
                pl.BlockSpec((1, NVIR), lambda i, c, p: (0, 0)),
            ),
        ),
        compiler_params=pltpu.CompilerParams(dimension_semantics=("arbitrary",)),
        name="residual",
    )(core, pair_energy, l_own, l_oth, other_terms, row_energy, col_energy)


def shards(amplitudes, factors, kernel, other_terms, virt_energy, pair_energy):
    core_id = lax.axis_index("c")
    core = core_id.astype(jnp.int32).reshape((1,))

    x_pad = jnp.pad(factors, ((0, PAD - ROW), (0, 0)))
    x_ranks = lax.all_gather(x_pad, "z", axis=0)
    x_all = lax.all_gather(x_ranks, XY, axis=0)

    t_cols = jnp.pad(amplitudes, ((0, 0), (0, PAD - ROW), (0, PAD - ROW)))
    t_cols = jnp.transpose(t_cols, (2, 0, 1)).reshape(PAD, PAIRS * PAD)
    t_cols, _ = lax.optimization_barrier((t_cols, x_ranks))
    t_own = lax.all_gather(t_cols, "z", axis=0, tiled=True)
    t_oth = core_swap(t_own)

    x_many = jnp.broadcast_to(x_pad[None], (NV, PAD, BLK))
    x_many, _ = lax.optimization_barrier((x_many, t_own))
    xq = lax.all_to_all(x_many, XY, split_axis=0, concat_axis=0, tiled=True)
    x_rows = xq[:, :ROW].reshape(NVIR, BLK)

    h_msg = make_half(core, t_own, t_oth, xq.reshape(NZ, NC, PAD, BLK))
    h_own = lax.all_to_all(h_msg, XY, split_axis=0, concat_axis=0, tiled=True)
    h_own = h_own.reshape(NV * PAD, PAIRS * QC)
    h_oth = core_swap(h_own)

    z_cols = kernel.T.reshape(NV, QC, BLK)
    z_all = lax.all_to_all(z_cols, XY, split_axis=0, concat_axis=0, tiled=True)
    z_all = z_all.reshape(NZ, NC, QC, BLK)
    z_oth = core_swap(lax.dynamic_index_in_dim(z_all, 1 - core_id, 1, keepdims=False))

    b_own, b_send = make_main(
        core, h_own, h_oth, x_all.reshape(NV, NZ, PAD, BLK), z_all, z_oth
    )
    b_sum = (b_own + core_swap(b_send).astype(F32)).astype(BF)
    b_all = lax.all_to_all(
        b_sum.reshape(NV, PAD, PAIRS * QC), XY, split_axis=0, concat_axis=0, tiled=True
    )

    l_own, l_send = make_ladder(core, b_all, x_rows)
    l_sum = (l_own + core_swap(l_send).astype(F32)).astype(BF)
    l_parts = lax.all_to_all(
        l_sum.reshape(NZ, PAD // 2, NVIR), "z", split_axis=0, concat_axis=0, tiled=True
    )
    l_chunk = jnp.sum(l_parts.astype(F32), axis=0).astype(BF)
    l_mine = lax.all_gather(l_chunk, "z", axis=0, tiled=True)
    l_rest = core_swap(l_mine)

    row_energy = lax.dynamic_slice_in_dim(virt_energy, lax.axis_index(XY) * ROW, ROW, 0)
    residual, squares = make_final(
        core,
        pair_energy,
        l_mine.reshape(4, PAD, NVIR),
        l_rest.reshape(4, PAD, NVIR),
        other_terms,
        row_energy[:, None],
        virt_energy[None, :],
    )
    total = jnp.broadcast_to(jnp.sum(squares), (NV, 8, LANE))
    totals = lax.all_to_all(total, XY, split_axis=0, concat_axis=0, tiled=True)
    count = PAIRS * NVIR * NVIR
    update_rms = jnp.sqrt(jnp.sum(totals[:, 0, 0]) / count + epsilon)
    return residual, update_rms


def solution(mesh):
    torus = Mesh(mesh.devices.reshape(NX, NY, NZ, NC), AXES)
    return jax.shard_map(
        shards,
        mesh=torus,
        in_specs=(
            P(None, XY, RANK),
            P(XY, RANK),
            P(XY, RANK),
            P(None, XY, None),
            P(),
            P(),
        ),
        out_specs=(P(None, XY, None), P()),
        check_vma=False,
    )
```

```python
import jax
import jax.numpy as jnp
from jax import lax
from jax.experimental import pallas as pl
from jax.experimental.pallas import tpu as pltpu
from jax.sharding import Mesh
from jax.sharding import PartitionSpec as P

AXES = ("x", "y", "z", "c")
XY = ("x", "y")
RANK = ("z", "c")
BF = jnp.bfloat16
F32 = jnp.float32
epsilon = 1e-06

NX, NY, NZ, NC = 4, 4, 8, 2
NV = NX * NY
PAIRS = 8
ROW = 75
PAD = 80
BLK = 512
QC = 32
NVIR = 1200
LANE = 128
HALF = PAD // 2
CHUNK = 5
WIDE = 1280


def core_swap(value):
    return lax.ppermute(value, "c", [(0, 1), (1, 0)])


def regroup(tiles, want):
    out = None
    lane = lax.broadcasted_iota(jnp.int32, (PAD, LANE), 1) // QC
    for group, tile in enumerate(tiles):
        shift = ((group - want) * QC) % LANE
        moved = pltpu.roll(tile, shift, 1) if shift else tile
        out = moved if out is None else jnp.where(lane == group, moved, out)
    return out


def half_kernel(core_ref, own_ref, oth_ref, xz_ref, out_ref, acc_ref):
    core = core_ref[0]
    dims = (((0,), (0,)), ((), ()))
    x_own = xz_ref[:, core, :PAD, :].reshape(NZ * PAD, BLK)
    x_oth = xz_ref[:, 1 - core, :PAD, :].reshape(NZ * PAD, BLK)
    acc_ref[...] = lax.dot_general(
        own_ref[...], x_own, dims, preferred_element_type=F32
    ) + lax.dot_general(oth_ref[...], x_oth, dims, preferred_element_type=F32)
    for xx in range(NX):
        for half in range(2):
            tiles = [
                acc_ref[pl.ds((half * 4 + g) * PAD, PAD), pl.ds(xx * LANE, LANE)]
                for g in range(4)
            ]
            for yy in range(NY):
                out_ref[xx * NY + yy, :, pl.ds(half * LANE, LANE)] = regroup(tiles, yy).astype(BF)


def make_half(place, t_own, t_oth, xz):
    return pl.pallas_call(
        half_kernel,
        out_shape=jax.ShapeDtypeStruct((NV, PAD, PAIRS * QC), BF),
        in_specs=[pl.BlockSpec(memory_space=pltpu.SMEM)]
        + [pl.BlockSpec(memory_space=pltpu.VMEM)] * 3,
        scratch_shapes=[pltpu.VMEM((PAIRS * PAD, BLK), F32)],
        name="half",
    )(place, t_own, t_oth, xz)


def main_kernel(
    place_ref, ho_ref, hx_ref, xq_ref, x_ref, zo_ref, zx_ref, bo_ref, bx_ref, h_ref, acc_ref
):
    step = pl.program_id(0)
    half_m = PAIRS * QC

    def block(x):
        coupled = jnp.dot(h_ref[...], x, preferred_element_type=F32)
        z_own = zo_ref[0, 0, PAD:, :].reshape(1, QC, BLK).astype(F32)
        z_oth = zx_ref[...].reshape(1, QC, BLK).astype(F32)
        c_own = coupled[:half_m].reshape(PAIRS, QC, BLK) * z_own
        c_oth = coupled[half_m:].reshape(PAIRS, QC, BLK) * z_oth
        w = jnp.concatenate(
            [c_own.reshape(half_m, BLK), c_oth.reshape(half_m, BLK)], axis=0
        ).astype(BF)
        return lax.dot_general(x, w, (((1,), (1,)), ((), ())), preferred_element_type=F32)

    @pl.when(step == 0)
    def _():
        h_ref[pl.ds(0, half_m), :] = ho_ref[...].astype(F32).T.astype(BF)
        h_ref[pl.ds(half_m, half_m), :] = hx_ref[...].astype(F32).T.astype(BF)
        acc_ref[...] = block(xq_ref[:, :PAD, :].reshape(NV * PAD, BLK))

    @pl.when(step > 0)
    def _():
        acc_ref[...] += block(x_ref[...].reshape(NV * PAD, BLK))

    @pl.when(step == NZ - 1)
    def _():
        bo_ref[...] = acc_ref[:, :half_m]
        bx_ref[...] = acc_ref[:, half_m:].astype(BF)


def make_main(place, h_own, h_oth, xz, x_all, z_oth):
    rows = NV * PAD
    half_m = PAIRS * QC
    return pl.pallas_call(
        main_kernel,
        out_shape=(
            jax.ShapeDtypeStruct((rows, half_m), F32),
            jax.ShapeDtypeStruct((rows, half_m), BF),
        ),
        grid_spec=pltpu.PrefetchScalarGridSpec(
            num_scalar_prefetch=1,
            grid=(NZ,),
            in_specs=[
                pl.BlockSpec((rows, half_m), lambda k, p: (0, 0)),
                pl.BlockSpec((rows, half_m), lambda k, p: (0, 0)),
                pl.BlockSpec((NV, PAD + QC, BLK), lambda k, p: (0, 0, 0)),
                pl.BlockSpec((NV, 1, PAD, BLK), lambda k, p: (0, jnp.maximum(k - 1, 0), 0, 0)),
                pl.BlockSpec((1, 1, PAD + QC, BLK), lambda k, p: ((p[1] + k) % NZ, p[0], 0, 0)),
                pl.BlockSpec((1, QC, BLK), lambda k, p: ((p[1] + k) % NZ, 0, 0)),
            ],
            out_specs=(
                pl.BlockSpec((rows, half_m), lambda k, p: (0, 0)),
                pl.BlockSpec((rows, half_m), lambda k, p: (0, 0)),
            ),
            scratch_shapes=[
                pltpu.VMEM((2 * half_m, rows), BF),
                pltpu.VMEM((rows, 2 * half_m), F32),
            ],
        ),
        compiler_params=pltpu.CompilerParams(dimension_semantics=("arbitrary",)),
        cost_estimate=pl.CostEstimate(
            flops=4 * 512 * 1280 * 4096, bytes_accessed=14_000_000, transcendentals=0
        ),
        name="ladder_core",
    )(place, h_own, h_oth, xz, x_all, xz.reshape(NZ, NC, PAD + QC, BLK), z_oth)


def ladder_kernel(place_ref, b_ref, x_ref, own_ref, oth_ref, g_ref):
    core = place_ref[0]
    for xx in range(NX):
        for half in range(2):
            tiles = [
                b_ref[xx * NY + yy, :, pl.ds(half * LANE, LANE)].astype(F32) for yy in range(NY)
            ]
            for g in range(4):
                g_ref[xx, pl.ds(half * 4 + g, PAD, stride=PAIRS), :] = regroup(tiles, g)
    dims = (((1,), (1,)), ((), ()))
    rows = HALF * PAIRS

    def gathered(which):
        start = pl.multiple_of(which * rows, rows)
        return jnp.concatenate([g_ref[xx, pl.ds(start, rows), :] for xx in range(NX)], axis=1)

    own = gathered(core).astype(BF)
    oth = gathered(1 - core).astype(BF)
    own_ref[...] = lax.dot_general(own, x_ref[...], dims, preferred_element_type=F32)
    oth_ref[...] = lax.dot_general(oth, x_ref[...], dims, preferred_element_type=F32).astype(BF)


def make_ladder(place, b_all, x_rows):
    return pl.pallas_call(
        ladder_kernel,
        out_shape=(
            jax.ShapeDtypeStruct((HALF * PAIRS, NVIR), F32),
            jax.ShapeDtypeStruct((HALF * PAIRS, NVIR), BF),
        ),
        in_specs=[pl.BlockSpec(memory_space=pltpu.SMEM)]
        + [pl.BlockSpec(memory_space=pltpu.VMEM)] * 2,
        scratch_shapes=[pltpu.VMEM((NX, PAIRS * PAD, LANE), F32)],
        name="ladder_rank",
    )(place, b_all, x_rows)


def chunk_kernel(place_ref, parts_ref, other_ref, col_ref, low_ref, out_ref):
    total = jnp.sum(parts_ref[...].astype(F32), axis=0)
    res = total + other_ref[...].reshape(CHUNK * PAIRS, NVIR)
    upd = res / (low_ref[...] + col_ref[...])
    squares = jnp.sum(upd * upd, axis=1, keepdims=True)
    squares = jnp.sum(squares, axis=0, keepdims=True)
    real = NC * NZ - 1
    squares = jnp.where(place_ref[2] < real, squares, 0.0)
    high = squares.astype(BF)
    rest = squares - high.astype(F32)
    mid = rest.astype(BF)
    low = (rest - mid.astype(F32)).astype(BF)
    out_ref[:, :NVIR] = total.astype(BF)
    lanes = WIDE - NVIR
    lane = lax.broadcasted_iota(jnp.int32, (CHUNK * PAIRS, lanes), 1)
    row = lax.broadcasted_iota(jnp.int32, (CHUNK * PAIRS, lanes), 0)
    kept = jnp.where(
        lane == 0, high.astype(F32), jnp.where(lane == 1, mid.astype(F32), low.astype(F32))
    )
    kept = jnp.where((row == 0) & (lane < 3), kept, 0.0)
    out_ref[:, NVIR:] = kept.astype(BF)


def make_chunk(place, parts, other_rows, col_energy, low_energy):
    last = ROW // CHUNK - 1
    return pl.pallas_call(
        chunk_kernel,
        out_shape=jax.ShapeDtypeStruct((CHUNK * PAIRS, WIDE), BF),
        grid_spec=pltpu.PrefetchScalarGridSpec(
            num_scalar_prefetch=1,
            grid=(1,),
            in_specs=[
                pl.BlockSpec((NZ, CHUNK * PAIRS, NVIR), lambda k, p: (0, 0, 0)),
                pl.BlockSpec((CHUNK, PAIRS, NVIR), lambda k, p: (jnp.minimum(p[2], last), 0, 0)),
                pl.BlockSpec((1, NVIR), lambda k, p: (0, 0)),
                pl.BlockSpec((CHUNK * PAIRS, 1), lambda k, p: (jnp.minimum(p[2], last), 0)),
            ],
            out_specs=pl.BlockSpec((CHUNK * PAIRS, WIDE), lambda k, p: (0, 0)),
        ),
        name="chunk",
    )(place, parts, other_rows, col_energy, low_energy)


def final_kernel(place_ref, own_ref, oth_ref, other_ref, out_ref):
    def fill(first, second):
        top = first[:, :NVIR].astype(F32).reshape(HALF, PAIRS, NVIR)
        out_ref[:HALF] = other_ref[:HALF] + top
        left = ROW - HALF
        end = second[: left * PAIRS, :NVIR].astype(F32).reshape(left, PAIRS, NVIR)
        out_ref[HALF:] = other_ref[HALF:] + end

    @pl.when(place_ref[0] == 0)
    def _():
        fill(own_ref, oth_ref)

    @pl.when(place_ref[0] == 1)
    def _():
        fill(oth_ref, own_ref)


def make_final(place, l_own, l_oth, other_rows):
    return pl.pallas_call(
        final_kernel,
        out_shape=jax.ShapeDtypeStruct((ROW, PAIRS, NVIR), F32),
        in_specs=[pl.BlockSpec(memory_space=pltpu.SMEM)]
        + [pl.BlockSpec(memory_space=pltpu.VMEM)] * 3,
        name="residual",
    )(place, l_own, l_oth, other_rows)


def shards(amplitudes, factors, kernel, other_terms, virt_energy, pair_energy):
    core = lax.axis_index("c").astype(jnp.int32)
    level = lax.axis_index("z").astype(jnp.int32)
    place = jnp.stack([core, level, core * NZ + level])

    x_pad = jnp.pad(factors, ((0, PAD - ROW), (0, 0)))
    x_far = [
        lax.ppermute(x_pad, "z", [(s, (s - j) % NZ) for s in range(NZ)]) for j in range(1, NZ)
    ]
    x_far = jnp.stack(x_far)
    x_all = lax.all_gather(x_far, XY, axis=0)

    z_cols = kernel.T.reshape(NV, QC, BLK)
    xz = jnp.concatenate([jnp.broadcast_to(x_pad[None], (NV, PAD, BLK)), z_cols], axis=1)
    t_cols = jnp.pad(amplitudes, ((0, 0), (0, PAD - ROW), (0, PAD - ROW)))
    t_cols = jnp.transpose(t_cols, (2, 0, 1)).reshape(PAD, PAIRS * PAD)
    t_cols, xz, _ = lax.optimization_barrier((t_cols, xz, x_far))
    xz = lax.all_to_all(xz, XY, split_axis=0, concat_axis=0, tiled=True)
    t_own = lax.all_gather(t_cols, "z", axis=0, tiled=True)
    t_oth = core_swap(t_own)
    x_rows = xz[:, :ROW].reshape(NVIR, BLK)

    h_msg = make_half(place, t_own, t_oth, xz.reshape(NZ, NC, PAD + QC, BLK))
    h_own = lax.all_to_all(h_msg, XY, split_axis=0, concat_axis=0, tiled=True)
    h_own = h_own.reshape(NV * PAD, PAIRS * QC)
    h_oth = core_swap(h_own)
    z_all = xz.reshape(NZ, NC, PAD + QC, BLK)
    z_oth = lax.dynamic_index_in_dim(z_all, 1 - core, 1, keepdims=False)[:, PAD:]
    z_oth = core_swap(z_oth)

    b_own, b_send = make_main(place, h_own, h_oth, xz, x_all, z_oth)
    b_sum = (b_own + core_swap(b_send).astype(F32)).astype(BF)
    b_all = lax.all_to_all(
        b_sum.reshape(NV, PAD, PAIRS * QC), XY, split_axis=0, concat_axis=0, tiled=True
    )

    l_own, l_send = make_ladder(place, b_all, x_rows)
    l_sum = (l_own + core_swap(l_send).astype(F32)).astype(BF)
    l_parts = lax.all_to_all(
        l_sum.reshape(NZ, CHUNK * PAIRS, NVIR), "z", split_axis=0, concat_axis=0, tiled=True
    )
    other_rows = jnp.transpose(other_terms, (1, 0, 2))
    row_energy = lax.dynamic_slice_in_dim(virt_energy, lax.axis_index(XY) * ROW, ROW, 0)
    low_energy = (row_energy[:, None] - pair_energy[None, :]).reshape(ROW * PAIRS, 1)
    chunk = make_chunk(place, l_parts, other_rows, virt_energy[None, :], low_energy)
    l_mine = lax.all_gather(chunk, "z", axis=0, tiled=True)
    l_rest = core_swap(l_mine)

    marks = jnp.concatenate([l_mine, l_rest]).reshape(NC * NZ, CHUNK * PAIRS, WIDE)
    squares = jnp.sum(marks[:, 0, NVIR : NVIR + 3].astype(F32))
    total = jnp.broadcast_to(squares, (NV, 8, LANE))
    totals = lax.all_to_all(total, XY, split_axis=0, concat_axis=0, tiled=True)
    residual = jnp.transpose(make_final(place, l_mine, l_rest, other_rows), (1, 0, 2))
    count = PAIRS * NVIR * NVIR
    update_rms = jnp.sqrt(jnp.sum(totals[:, 0, 0]) / count + epsilon)
    return residual, update_rms


def solution(mesh):
    torus = Mesh(mesh.devices.reshape(NX, NY, NZ, NC), AXES)
    return jax.shard_map(
        shards,
        mesh=torus,
        in_specs=(
            P(None, XY, RANK),
            P(XY, RANK),
            P(XY, RANK),
            P(None, XY, None),
            P(),
            P(),
        ),
        out_specs=(P(None, XY, None), P()),
        check_vma=False,
    )
```

```python
import jax
import jax.numpy as jnp
from jax import lax
from jax.experimental import pallas as pl
from jax.experimental.pallas import tpu as pltpu
from jax.sharding import Mesh
from jax.sharding import PartitionSpec as P

AXES = ("x", "y", "z", "c")
XY = ("x", "y")
RANK = ("z", "c")
BF = jnp.bfloat16
F32 = jnp.float32
epsilon = 1e-06

NX, NY, NZ, NC = 4, 4, 8, 2
NV = NX * NY
PAIRS = 8
ROW = 75
PAD = 80
BLK = 512
QC = 32
NVIR = 1200
LANE = 128
HALF = PAD // 2
CHUNK = 5
WIDE = 1280


def core_swap(value):
    return lax.ppermute(value, "c", [(0, 1), (1, 0)])


def regroup(tiles, want):
    out = None
    lane = lax.broadcasted_iota(jnp.int32, (PAD, LANE), 1) // QC
    for group, tile in enumerate(tiles):
        shift = ((group - want) * QC) % LANE
        moved = pltpu.roll(tile, shift, 1) if shift else tile
        out = moved if out is None else jnp.where(lane == group, moved, out)
    return out


def half_kernel(core_ref, own_ref, oth_ref, xz_ref, out_ref, acc_ref):
    core = core_ref[0]
    dims = (((0,), (0,)), ((), ()))
    x_own = xz_ref[:, core, :PAD, :].reshape(NZ * PAD, BLK)
    x_oth = xz_ref[:, 1 - core, :PAD, :].reshape(NZ * PAD, BLK)
    acc_ref[...] = lax.dot_general(
        own_ref[...], x_own, dims, preferred_element_type=F32
    ) + lax.dot_general(oth_ref[...], x_oth, dims, preferred_element_type=F32)
    for xx in range(NX):
        for half in range(2):
            tiles = [
                acc_ref[pl.ds((half * 4 + g) * PAD, PAD), pl.ds(xx * LANE, LANE)]
                for g in range(4)
            ]
            for yy in range(NY):
                out_ref[xx * NY + yy, :, pl.ds(half * LANE, LANE)] = regroup(tiles, yy).astype(BF)


def make_half(place, t_own, t_oth, xz):
    return pl.pallas_call(
        half_kernel,
        out_shape=jax.ShapeDtypeStruct((NV, PAD, PAIRS * QC), BF),
        in_specs=[pl.BlockSpec(memory_space=pltpu.SMEM)]
        + [pl.BlockSpec(memory_space=pltpu.VMEM)] * 3,
        scratch_shapes=[pltpu.VMEM((PAIRS * PAD, BLK), F32)],
        name="half",
    )(place, t_own, t_oth, xz)


def level_of(step, place):
    far = jnp.where(step == 2, NZ - 1, jnp.where(step > 2, step - 1, step))
    return (place[1] + far) % NZ


def main_kernel(
    place_ref,
    ho_ref,
    hx_ref,
    xq_ref,
    xu_ref,
    xd_ref,
    x_ref,
    zo_ref,
    zx_ref,
    bo_ref,
    bx_ref,
    h_ref,
    acc_ref,
    now_ref,
):
    step = pl.program_id(0)
    half_m = PAIRS * QC

    def block():
        x = now_ref[...]
        coupled = jnp.dot(h_ref[...], x, preferred_element_type=F32)
        z_own = zo_ref[0, 0, PAD:, :].reshape(1, QC, BLK).astype(F32)
        z_oth = zx_ref[...].reshape(1, QC, BLK).astype(F32)
        c_own = coupled[:half_m].reshape(PAIRS, QC, BLK) * z_own
        c_oth = coupled[half_m:].reshape(PAIRS, QC, BLK) * z_oth
        w = jnp.concatenate(
            [c_own.reshape(half_m, BLK), c_oth.reshape(half_m, BLK)], axis=0
        ).astype(BF)
        return lax.dot_general(x, w, (((1,), (1,)), ((), ())), preferred_element_type=F32)

    @pl.when(step == 0)
    def _():
        h_ref[pl.ds(0, half_m), :] = ho_ref[...].astype(F32).T.astype(BF)
        h_ref[pl.ds(half_m, half_m), :] = hx_ref[...].astype(F32).T.astype(BF)
        acc_ref[...] = jnp.zeros_like(acc_ref)
        now_ref[...] = xq_ref[:, :PAD, :].reshape(NV * PAD, BLK)

    @pl.when(step == 1)
    def _():
        now_ref[...] = xu_ref[...].reshape(NV * PAD, BLK)

    @pl.when(step == 2)
    def _():
        now_ref[...] = xd_ref[...].reshape(NV * PAD, BLK)

    @pl.when(step > 2)
    def _():
        now_ref[...] = x_ref[...].reshape(NV * PAD, BLK)

    acc_ref[...] += block()

    @pl.when(step == NZ - 1)
    def _():
        bo_ref[...] = acc_ref[:, :half_m]
        bx_ref[...] = acc_ref[:, half_m:].astype(BF)


def make_main(place, h_own, h_oth, xz, x_up, x_down, x_all, z_oth):
    rows = NV * PAD
    half_m = PAIRS * QC
    return pl.pallas_call(
        main_kernel,
        out_shape=(
            jax.ShapeDtypeStruct((rows, half_m), F32),
            jax.ShapeDtypeStruct((rows, half_m), BF),
        ),
        grid_spec=pltpu.PrefetchScalarGridSpec(
            num_scalar_prefetch=1,
            grid=(NZ,),
            in_specs=[
                pl.BlockSpec((rows, half_m), lambda k, p: (0, 0)),
                pl.BlockSpec((rows, half_m), lambda k, p: (0, 0)),
                pl.BlockSpec((NV, PAD + QC, BLK), lambda k, p: (0, 0, 0)),
                pl.BlockSpec((NV, PAD, BLK), lambda k, p: (0, 0, 0)),
                pl.BlockSpec((NV, PAD, BLK), lambda k, p: (0, 0, 0)),
                pl.BlockSpec((NV, 1, PAD, BLK), lambda k, p: (0, jnp.maximum(k - 3, 0), 0, 0)),
                pl.BlockSpec((1, 1, PAD + QC, BLK), lambda k, p: (level_of(k, p), p[0], 0, 0)),
                pl.BlockSpec((1, QC, BLK), lambda k, p: (level_of(k, p), 0, 0)),
            ],
            out_specs=(
                pl.BlockSpec((rows, half_m), lambda k, p: (0, 0)),
                pl.BlockSpec((rows, half_m), lambda k, p: (0, 0)),
            ),
            scratch_shapes=[
                pltpu.VMEM((2 * half_m, rows), BF),
                pltpu.VMEM((rows, 2 * half_m), F32),
                pltpu.VMEM((rows, BLK), BF),
            ],
        ),
        compiler_params=pltpu.CompilerParams(dimension_semantics=("arbitrary",)),
        cost_estimate=pl.CostEstimate(
            flops=4 * 512 * 1280 * 4096, bytes_accessed=14_000_000, transcendentals=0
        ),
        name="ladder_core",
    )(place, h_own, h_oth, xz, x_up, x_down, x_all, xz.reshape(NZ, NC, PAD + QC, BLK), z_oth)


def ladder_kernel(place_ref, b_ref, x_ref, own_ref, oth_ref, g_ref):
    core = place_ref[0]
    for xx in range(NX):
        for half in range(2):
            tiles = [
                b_ref[xx * NY + yy, :, pl.ds(half * LANE, LANE)].astype(F32) for yy in range(NY)
            ]
            for g in range(4):
                g_ref[xx, pl.ds(half * 4 + g, PAD, stride=PAIRS), :] = regroup(tiles, g)
    dims = (((1,), (1,)), ((), ()))
    rows = HALF * PAIRS

    def gathered(which):
        start = pl.multiple_of(which * rows, rows)
        return jnp.concatenate([g_ref[xx, pl.ds(start, rows), :] for xx in range(NX)], axis=1)

    own = gathered(core).astype(BF)
    oth = gathered(1 - core).astype(BF)
    own_ref[...] = lax.dot_general(own, x_ref[...], dims, preferred_element_type=F32)
    oth_ref[...] = lax.dot_general(oth, x_ref[...], dims, preferred_element_type=F32).astype(BF)


def make_ladder(place, b_all, x_rows):
    return pl.pallas_call(
        ladder_kernel,
        out_shape=(
            jax.ShapeDtypeStruct((HALF * PAIRS, NVIR), F32),
            jax.ShapeDtypeStruct((HALF * PAIRS, NVIR), BF),
        ),
        in_specs=[pl.BlockSpec(memory_space=pltpu.SMEM)]
        + [pl.BlockSpec(memory_space=pltpu.VMEM)] * 2,
        scratch_shapes=[pltpu.VMEM((NX, PAIRS * PAD, LANE), F32)],
        name="ladder_rank",
    )(place, b_all, x_rows)


def chunk_kernel(place_ref, parts_ref, other_ref, col_ref, low_ref, out_ref):
    total = jnp.sum(parts_ref[...].astype(F32), axis=0)
    res = total + other_ref[...].reshape(CHUNK * PAIRS, NVIR)
    upd = res / (low_ref[...] + col_ref[...])
    squares = jnp.sum(upd * upd, axis=1, keepdims=True)
    squares = jnp.sum(squares, axis=0, keepdims=True)
    real = NC * NZ - 1
    squares = jnp.where(place_ref[2] < real, squares, 0.0)
    high = squares.astype(BF)
    rest = squares - high.astype(F32)
    mid = rest.astype(BF)
    low = (rest - mid.astype(F32)).astype(BF)
    out_ref[:, :NVIR] = total.astype(BF)
    lanes = WIDE - NVIR
    lane = lax.broadcasted_iota(jnp.int32, (CHUNK * PAIRS, lanes), 1)
    row = lax.broadcasted_iota(jnp.int32, (CHUNK * PAIRS, lanes), 0)
    kept = jnp.where(
        lane == 0, high.astype(F32), jnp.where(lane == 1, mid.astype(F32), low.astype(F32))
    )
    kept = jnp.where((row == 0) & (lane < 3), kept, 0.0)
    out_ref[:, NVIR:] = kept.astype(BF)


def make_chunk(place, parts, other_rows, col_energy, low_energy):
    last = ROW // CHUNK - 1
    return pl.pallas_call(
        chunk_kernel,
        out_shape=jax.ShapeDtypeStruct((CHUNK * PAIRS, WIDE), BF),
        grid_spec=pltpu.PrefetchScalarGridSpec(
            num_scalar_prefetch=1,
            grid=(1,),
            in_specs=[
                pl.BlockSpec((NZ, CHUNK * PAIRS, NVIR), lambda k, p: (0, 0, 0)),
                pl.BlockSpec((CHUNK, PAIRS, NVIR), lambda k, p: (jnp.minimum(p[2], last), 0, 0)),
                pl.BlockSpec((1, NVIR), lambda k, p: (0, 0)),
                pl.BlockSpec((CHUNK * PAIRS, 1), lambda k, p: (jnp.minimum(p[2], last), 0)),
            ],
            out_specs=pl.BlockSpec((CHUNK * PAIRS, WIDE), lambda k, p: (0, 0)),
        ),
        name="chunk",
    )(place, parts, other_rows, col_energy, low_energy)


def final_kernel(place_ref, own_ref, oth_ref, other_ref, out_ref):
    def fill(first, second):
        top = first[:, :NVIR].astype(F32).reshape(HALF, PAIRS, NVIR)
        out_ref[:HALF] = other_ref[:HALF] + top
        left = ROW - HALF
        end = second[: left * PAIRS, :NVIR].astype(F32).reshape(left, PAIRS, NVIR)
        out_ref[HALF:] = other_ref[HALF:] + end

    @pl.when(place_ref[0] == 0)
    def _():
        fill(own_ref, oth_ref)

    @pl.when(place_ref[0] == 1)
    def _():
        fill(oth_ref, own_ref)


def make_final(place, l_own, l_oth, other_rows):
    return pl.pallas_call(
        final_kernel,
        out_shape=jax.ShapeDtypeStruct((ROW, PAIRS, NVIR), F32),
        in_specs=[pl.BlockSpec(memory_space=pltpu.SMEM)]
        + [pl.BlockSpec(memory_space=pltpu.VMEM)] * 3,
        name="residual",
    )(place, l_own, l_oth, other_rows)


def shards(amplitudes, factors, kernel, other_terms, virt_energy, pair_energy):
    core = lax.axis_index("c").astype(jnp.int32)
    level = lax.axis_index("z").astype(jnp.int32)
    place = jnp.stack([core, level, core * NZ + level])

    x_pad = jnp.pad(factors, ((0, PAD - ROW), (0, 0)))
    x_far = [
        lax.ppermute(x_pad, "z", [(s, (s - j) % NZ) for s in range(NZ)]) for j in range(2, NZ - 1)
    ]
    x_far = jnp.stack(x_far)
    x_all = lax.all_gather(x_far, XY, axis=0)

    z_cols = kernel.T.reshape(NV, QC, BLK)
    xz = jnp.concatenate([jnp.broadcast_to(x_pad[None], (NV, PAD, BLK)), z_cols], axis=1)
    t_cols = jnp.pad(amplitudes, ((0, 0), (0, PAD - ROW), (0, PAD - ROW)))
    t_cols = jnp.transpose(t_cols, (2, 0, 1)).reshape(PAD, PAIRS * PAD)
    t_cols, _ = lax.optimization_barrier((t_cols, x_far))
    xz = lax.all_to_all(xz, XY, split_axis=0, concat_axis=0, tiled=True)
    t_own = lax.all_gather(t_cols, "z", axis=0, tiled=True)
    t_oth = core_swap(t_own)
    x_own = xz[:, :PAD]
    x_up = lax.ppermute(x_own, "z", [(s, (s - 1) % NZ) for s in range(NZ)])
    x_down = lax.ppermute(x_own, "z", [(s, (s + 1) % NZ) for s in range(NZ)])
    x_rows = xz[:, :ROW].reshape(NVIR, BLK)

    h_msg = make_half(place, t_own, t_oth, xz.reshape(NZ, NC, PAD + QC, BLK))
    h_own = lax.all_to_all(h_msg, XY, split_axis=0, concat_axis=0, tiled=True)
    h_own = h_own.reshape(NV * PAD, PAIRS * QC)
    h_oth = core_swap(h_own)
    z_all = xz.reshape(NZ, NC, PAD + QC, BLK)
    z_oth = lax.dynamic_index_in_dim(z_all, 1 - core, 1, keepdims=False)[:, PAD:]
    z_oth = core_swap(z_oth)

    b_own, b_send = make_main(place, h_own, h_oth, xz, x_up, x_down, x_all, z_oth)
    b_sum = (b_own + core_swap(b_send).astype(F32)).astype(BF)
    b_all = lax.all_to_all(
        b_sum.reshape(NV, PAD, PAIRS * QC), XY, split_axis=0, concat_axis=0, tiled=True
    )

    l_own, l_send = make_ladder(place, b_all, x_rows)
    l_sum = (l_own + core_swap(l_send).astype(F32)).astype(BF)
    l_parts = lax.all_to_all(
        l_sum.reshape(NZ, CHUNK * PAIRS, NVIR), "z", split_axis=0, concat_axis=0, tiled=True
    )
    other_rows = jnp.transpose(other_terms, (1, 0, 2))
    row_energy = lax.dynamic_slice_in_dim(virt_energy, lax.axis_index(XY) * ROW, ROW, 0)
    low_energy = (row_energy[:, None] - pair_energy[None, :]).reshape(ROW * PAIRS, 1)
    chunk = make_chunk(place, l_parts, other_rows, virt_energy[None, :], low_energy)
    l_mine = lax.all_gather(chunk, "z", axis=0, tiled=True)
    l_rest = core_swap(l_mine)

    marks = jnp.concatenate([l_mine, l_rest]).reshape(NC * NZ, CHUNK * PAIRS, WIDE)
    squares = jnp.sum(marks[:, 0, NVIR : NVIR + 3].astype(F32))
    total = jnp.broadcast_to(squares, (NV, 8, LANE))
    totals = lax.all_to_all(total, XY, split_axis=0, concat_axis=0, tiled=True)
    residual = jnp.transpose(make_final(place, l_mine, l_rest, other_rows), (1, 0, 2))
    count = PAIRS * NVIR * NVIR
    update_rms = jnp.sqrt(jnp.sum(totals[:, 0, 0]) / count + epsilon)
    return residual, update_rms


def solution(mesh):
    torus = Mesh(mesh.devices.reshape(NX, NY, NZ, NC), AXES)
    return jax.shard_map(
        shards,
        mesh=torus,
        in_specs=(
            P(None, XY, RANK),
            P(XY, RANK),
            P(XY, RANK),
            P(None, XY, None),
            P(),
            P(),
        ),
        out_specs=(P(None, XY, None), P()),
        check_vma=False,
    )
```

```python
import jax
import jax.numpy as jnp
from jax import lax
from jax.experimental import pallas as pl
from jax.experimental.pallas import tpu as pltpu
from jax.sharding import Mesh
from jax.sharding import PartitionSpec as P

AXES = ("x", "y", "z", "c")
XY = ("x", "y")
RANK = ("z", "c")
BF = jnp.bfloat16
F32 = jnp.float32
epsilon = 1e-06

NX, NY, NZ, NC = 4, 4, 8, 2
NV = NX * NY
PAIRS = 8
ROW = 75
PAD = 80
BLK = 512
QC = 32
NVIR = 1200
LANE = 128
HALF = PAD // 2
CHUNK = 5
WIDE = 1280


def core_swap(value):
    return lax.ppermute(value, "c", [(0, 1), (1, 0)])


def ring(shift):
    return [(s, (s + shift) % NZ) for s in range(NZ)]


def regroup(tiles, want):
    out = None
    lane = lax.broadcasted_iota(jnp.int32, (PAD, LANE), 1) // QC
    for group, tile in enumerate(tiles):
        shift = ((group - want) * QC) % LANE
        moved = pltpu.roll(tile, shift, 1) if shift else tile
        out = moved if out is None else jnp.where(lane == group, moved, out)
    return out


def half_kernel(core_ref, own_ref, oth_ref, xz_ref, out_ref, acc_ref):
    core = core_ref[0]
    dims = (((0,), (0,)), ((), ()))
    x_own = xz_ref[:, core, :PAD, :].reshape(NZ * PAD, BLK)
    x_oth = xz_ref[:, 1 - core, :PAD, :].reshape(NZ * PAD, BLK)
    acc_ref[...] = lax.dot_general(
        own_ref[...], x_own, dims, preferred_element_type=F32
    ) + lax.dot_general(oth_ref[...], x_oth, dims, preferred_element_type=F32)
    for xx in range(NX):
        for half in range(2):
            tiles = [
                acc_ref[pl.ds((half * 4 + g) * PAD, PAD), pl.ds(xx * LANE, LANE)]
                for g in range(4)
            ]
            for yy in range(NY):
                out_ref[xx * NY + yy, :, pl.ds(half * LANE, LANE)] = regroup(tiles, yy).astype(BF)


def make_half(place, t_own, t_oth, xz):
    return pl.pallas_call(
        half_kernel,
        out_shape=jax.ShapeDtypeStruct((NV, PAD, PAIRS * QC), BF),
        in_specs=[pl.BlockSpec(memory_space=pltpu.SMEM)]
        + [pl.BlockSpec(memory_space=pltpu.VMEM)] * 3,
        scratch_shapes=[pltpu.VMEM((PAIRS * PAD, BLK), F32)],
        name="half",
    )(place, t_own, t_oth, xz)


FIRST = (0, 1, NZ - 1, 3, 4, 5)
LAST = (2, NZ - 2)
HALF_M = PAIRS * QC


def back_block(h, x, z_own, z_oth):
    coupled = jnp.dot(h, x, preferred_element_type=F32)
    z_own = z_own.reshape(1, QC, BLK).astype(F32)
    z_oth = z_oth.reshape(1, QC, BLK).astype(F32)
    c_own = coupled[:HALF_M].reshape(PAIRS, QC, BLK) * z_own
    c_oth = coupled[HALF_M:].reshape(PAIRS, QC, BLK) * z_oth
    w = jnp.concatenate(
        [c_own.reshape(HALF_M, BLK), c_oth.reshape(HALF_M, BLK)], axis=0
    ).astype(BF)
    return lax.dot_general(x, w, (((1,), (1,)), ((), ())), preferred_element_type=F32)


def first_kernel(
    place_ref, ho_ref, hx_ref, xq_ref, xu_ref, xd_ref, x_ref, zo_ref, zx_ref, acc_ref, h_ref, now_ref
):
    step = pl.program_id(0)

    @pl.when(step == 0)
    def _():
        h_ref[pl.ds(0, HALF_M), :] = ho_ref[...].astype(F32).T.astype(BF)
        h_ref[pl.ds(HALF_M, HALF_M), :] = hx_ref[...].astype(F32).T.astype(BF)
        acc_ref[...] = jnp.zeros_like(acc_ref)
        now_ref[...] = xq_ref[:, :PAD, :].reshape(NV * PAD, BLK)

    @pl.when(step == 1)
    def _():
        now_ref[...] = xu_ref[...].reshape(NV * PAD, BLK)

    @pl.when(step == 2)
    def _():
        now_ref[...] = xd_ref[...].reshape(NV * PAD, BLK)

    @pl.when(step > 2)
    def _():
        now_ref[...] = x_ref[...].reshape(NV * PAD, BLK)

    acc_ref[...] += back_block(h_ref[...], now_ref[...], zo_ref[0, 0, PAD:, :], zx_ref[...])


def first_level(step, place):
    far = jnp.where(step == 2, NZ - 1, step)
    return (place[1] + far) % NZ


def make_first(place, h_own, h_oth, xz, x_up, x_down, x_all, z_oth):
    rows = NV * PAD
    whole = pl.BlockSpec((NV, PAD, BLK), lambda k, p: (0, 0, 0))
    return pl.pallas_call(
        first_kernel,
        out_shape=(
            jax.ShapeDtypeStruct((rows, 2 * HALF_M), F32),
            jax.ShapeDtypeStruct((2 * HALF_M, rows), BF),
        ),
        grid_spec=pltpu.PrefetchScalarGridSpec(
            num_scalar_prefetch=1,
            grid=(len(FIRST),),
            in_specs=[
                pl.BlockSpec((rows, HALF_M), lambda k, p: (0, 0)),
                pl.BlockSpec((rows, HALF_M), lambda k, p: (0, 0)),
                pl.BlockSpec((NV, PAD + QC, BLK), lambda k, p: (0, 0, 0)),
                whole,
                whole,
                pl.BlockSpec((NV, 1, PAD, BLK), lambda k, p: (0, jnp.maximum(k - 3, 0), 0, 0)),
                pl.BlockSpec((1, 1, PAD + QC, BLK), lambda k, p: (first_level(k, p), p[0], 0, 0)),
                pl.BlockSpec((1, QC, BLK), lambda k, p: (first_level(k, p), 0, 0)),
            ],
            out_specs=(
                pl.BlockSpec((rows, 2 * HALF_M), lambda k, p: (0, 0)),
                pl.BlockSpec((2 * HALF_M, rows), lambda k, p: (0, 0)),
            ),
            scratch_shapes=[pltpu.VMEM((rows, BLK), BF)],
        ),
        compiler_params=pltpu.CompilerParams(dimension_semantics=("arbitrary",)),
        cost_estimate=pl.CostEstimate(
            flops=4 * 512 * 1280 * 512 * len(FIRST), bytes_accessed=12_000_000, transcendentals=0
        ),
        name="core_first",
    )(place, h_own, h_oth, xz, x_up, x_down, x_all, xz.reshape(NZ, NC, PAD + QC, BLK), z_oth)


def last_kernel(
    place_ref, acc_ref, h_ref, xu_ref, xd_ref, zou_ref, zxu_ref, zod_ref, zxd_ref, bo_ref, bx_ref
):
    h = h_ref[...]
    up = xu_ref[...].reshape(NV * PAD, BLK)
    down = xd_ref[...].reshape(NV * PAD, BLK)
    total = acc_ref[...] + back_block(h, up, zou_ref[0, 0, PAD:, :], zxu_ref[...])
    total += back_block(h, down, zod_ref[0, 0, PAD:, :], zxd_ref[...])
    bo_ref[...] = total[:, :HALF_M]
    bx_ref[...] = total[:, HALF_M:].astype(BF)


def make_last(place, acc, h, x_up, x_down, xz, z_oth):
    rows = NV * PAD
    whole = pl.BlockSpec((NV, PAD, BLK), lambda k, p: (0, 0, 0))

    def z_specs(far):
        return [
            pl.BlockSpec((1, 1, PAD + QC, BLK), lambda k, p: ((p[1] + far) % NZ, p[0], 0, 0)),
            pl.BlockSpec((1, QC, BLK), lambda k, p: ((p[1] + far) % NZ, 0, 0)),
        ]

    z_all = xz.reshape(NZ, NC, PAD + QC, BLK)
    return pl.pallas_call(
        last_kernel,
        out_shape=(
            jax.ShapeDtypeStruct((rows, HALF_M), F32),
            jax.ShapeDtypeStruct((rows, HALF_M), BF),
        ),
        grid_spec=pltpu.PrefetchScalarGridSpec(
            num_scalar_prefetch=1,
            grid=(1,),
            in_specs=[
                pl.BlockSpec((rows, 2 * HALF_M), lambda k, p: (0, 0)),
                pl.BlockSpec((2 * HALF_M, rows), lambda k, p: (0, 0)),
                whole,
                whole,
            ]
            + z_specs(LAST[0])
            + z_specs(LAST[1]),
            out_specs=(
                pl.BlockSpec((rows, HALF_M), lambda k, p: (0, 0)),
                pl.BlockSpec((rows, HALF_M), lambda k, p: (0, 0)),
            ),
        ),
        compiler_params=pltpu.CompilerParams(dimension_semantics=("arbitrary",)),
        cost_estimate=pl.CostEstimate(
            flops=4 * 512 * 1280 * 512 * len(LAST), bytes_accessed=8_000_000, transcendentals=0
        ),
        name="core_last",
    )(place, acc, h, x_up, x_down, z_all, z_oth, z_all, z_oth)


def ladder_kernel(place_ref, b_ref, x_ref, own_ref, oth_ref, g_ref):
    core = place_ref[0]
    for xx in range(NX):
        for half in range(2):
            tiles = [
                b_ref[xx * NY + yy, :, pl.ds(half * LANE, LANE)].astype(F32) for yy in range(NY)
            ]
            for g in range(4):
                g_ref[xx, pl.ds(half * 4 + g, PAD, stride=PAIRS), :] = regroup(tiles, g)
    dims = (((1,), (1,)), ((), ()))
    rows = HALF * PAIRS

    def gathered(which):
        start = pl.multiple_of(which * rows, rows)
        return jnp.concatenate([g_ref[xx, pl.ds(start, rows), :] for xx in range(NX)], axis=1)

    own = gathered(core).astype(BF)
    oth = gathered(1 - core).astype(BF)
    own_ref[...] = lax.dot_general(own, x_ref[...], dims, preferred_element_type=F32)
    oth_ref[...] = lax.dot_general(oth, x_ref[...], dims, preferred_element_type=F32).astype(BF)


def make_ladder(place, b_all, x_rows):
    return pl.pallas_call(
        ladder_kernel,
        out_shape=(
            jax.ShapeDtypeStruct((HALF * PAIRS, NVIR), F32),
            jax.ShapeDtypeStruct((HALF * PAIRS, NVIR), BF),
        ),
        in_specs=[pl.BlockSpec(memory_space=pltpu.SMEM)]
        + [pl.BlockSpec(memory_space=pltpu.VMEM)] * 2,
        scratch_shapes=[pltpu.VMEM((NX, PAIRS * PAD, LANE), F32)],
        name="ladder_rank",
    )(place, b_all, x_rows)


def chunk_kernel(place_ref, parts_ref, other_ref, col_ref, low_ref, out_ref):
    total = jnp.sum(parts_ref[...].astype(F32), axis=0)
    res = total + other_ref[...].reshape(CHUNK * PAIRS, NVIR)
    upd = res / (low_ref[...] + col_ref[...])
    squares = jnp.sum(upd * upd, axis=1, keepdims=True)
    squares = jnp.sum(squares, axis=0, keepdims=True)
    real = NC * NZ - 1
    squares = jnp.where(place_ref[2] < real, squares, 0.0)
    high = squares.astype(BF)
    rest = squares - high.astype(F32)
    mid = rest.astype(BF)
    low = (rest - mid.astype(F32)).astype(BF)
    out_ref[:, :NVIR] = total.astype(BF)
    lanes = WIDE - NVIR
    lane = lax.broadcasted_iota(jnp.int32, (CHUNK * PAIRS, lanes), 1)
    row = lax.broadcasted_iota(jnp.int32, (CHUNK * PAIRS, lanes), 0)
    kept = jnp.where(
        lane == 0, high.astype(F32), jnp.where(lane == 1, mid.astype(F32), low.astype(F32))
    )
    kept = jnp.where((row == 0) & (lane < 3), kept, 0.0)
    out_ref[:, NVIR:] = kept.astype(BF)


def make_chunk(place, parts, other_rows, col_energy, low_energy):
    last = ROW // CHUNK - 1
    return pl.pallas_call(
        chunk_kernel,
        out_shape=jax.ShapeDtypeStruct((CHUNK * PAIRS, WIDE), BF),
        grid_spec=pltpu.PrefetchScalarGridSpec(
            num_scalar_prefetch=1,
            grid=(1,),
            in_specs=[
                pl.BlockSpec((NZ, CHUNK * PAIRS, NVIR), lambda k, p: (0, 0, 0)),
                pl.BlockSpec((CHUNK, PAIRS, NVIR), lambda k, p: (jnp.minimum(p[2], last), 0, 0)),
                pl.BlockSpec((1, NVIR), lambda k, p: (0, 0)),
                pl.BlockSpec((CHUNK * PAIRS, 1), lambda k, p: (jnp.minimum(p[2], last), 0)),
            ],
            out_specs=pl.BlockSpec((CHUNK * PAIRS, WIDE), lambda k, p: (0, 0)),
        ),
        name="chunk",
    )(place, parts, other_rows, col_energy, low_energy)


def final_kernel(place_ref, own_ref, oth_ref, other_ref, out_ref):
    def fill(first, second):
        top = first[:, :NVIR].astype(F32).reshape(HALF, PAIRS, NVIR)
        out_ref[:HALF] = other_ref[:HALF] + top
        left = ROW - HALF
        end = second[: left * PAIRS, :NVIR].astype(F32).reshape(left, PAIRS, NVIR)
        out_ref[HALF:] = other_ref[HALF:] + end

    @pl.when(place_ref[0] == 0)
    def _():
        fill(own_ref, oth_ref)

    @pl.when(place_ref[0] == 1)
    def _():
        fill(oth_ref, own_ref)


def make_final(place, l_own, l_oth, other_rows):
    return pl.pallas_call(
        final_kernel,
        out_shape=jax.ShapeDtypeStruct((ROW, PAIRS, NVIR), F32),
        in_specs=[pl.BlockSpec(memory_space=pltpu.SMEM)]
        + [pl.BlockSpec(memory_space=pltpu.VMEM)] * 3,
        name="residual",
    )(place, l_own, l_oth, other_rows)


def shards(amplitudes, factors, kernel, other_terms, virt_energy, pair_energy):
    core = lax.axis_index("c").astype(jnp.int32)
    level = lax.axis_index("z").astype(jnp.int32)
    place = jnp.stack([core, level, core * NZ + level])

    x_pad = jnp.pad(factors, ((0, PAD - ROW), (0, 0)))
    z_cols = kernel.T.reshape(NV, QC, BLK)
    xz = jnp.concatenate([jnp.broadcast_to(x_pad[None], (NV, PAD, BLK)), z_cols], axis=1)
    x_pad, xz = lax.optimization_barrier((x_pad, xz))
    with jax.named_scope("own"):
        xz = lax.all_to_all(xz, XY, split_axis=0, concat_axis=0, tiled=True)
    with jax.named_scope("far"):
        x_far = jnp.stack([lax.ppermute(x_pad, "z", ring(-j)) for j in FIRST[3:]])
    x_all = lax.all_gather(x_far, XY, axis=0)

    t_cols = jnp.pad(amplitudes, ((0, 0), (0, PAD - ROW), (0, PAD - ROW)))
    t_cols = jnp.transpose(t_cols, (2, 0, 1)).reshape(PAD, PAIRS * PAD)
    t_cols, _ = lax.optimization_barrier((t_cols, x_far))
    t_own = lax.all_gather(t_cols, "z", axis=0, tiled=True)
    t_oth = core_swap(t_own)
    x_own = xz[:, :PAD]
    with jax.named_scope("near"):
        x_up = lax.ppermute(x_own, "z", ring(-1))
        x_down = lax.ppermute(x_own, "z", ring(1))
    with jax.named_scope("next"):
        x_up2 = lax.ppermute(x_up, "z", ring(-1))
        x_down2 = lax.ppermute(x_down, "z", ring(1))
    x_rows = xz[:, :ROW].reshape(NVIR, BLK)

    h_msg = make_half(place, t_own, t_oth, xz.reshape(NZ, NC, PAD + QC, BLK))
    with jax.named_scope("spread"):
        h_own = lax.all_to_all(h_msg, XY, split_axis=0, concat_axis=0, tiled=True)
    h_own = h_own.reshape(NV * PAD, PAIRS * QC)
    h_oth = core_swap(h_own)
    z_all = xz.reshape(NZ, NC, PAD + QC, BLK)
    z_oth = lax.dynamic_index_in_dim(z_all, 1 - core, 1, keepdims=False)[:, PAD:]
    z_oth = core_swap(z_oth)

    acc, h = make_first(place, h_own, h_oth, xz, x_up, x_down, x_all, z_oth)
    b_own, b_send = make_last(place, acc, h, x_up2, x_down2, xz, z_oth)
    b_sum = (b_own + core_swap(b_send).astype(F32)).astype(BF)
    b_all = lax.all_to_all(
        b_sum.reshape(NV, PAD, PAIRS * QC), XY, split_axis=0, concat_axis=0, tiled=True
    )

    l_own, l_send = make_ladder(place, b_all, x_rows)
    l_sum = (l_own + core_swap(l_send).astype(F32)).astype(BF)
    l_parts = lax.all_to_all(
        l_sum.reshape(NZ, CHUNK * PAIRS, NVIR), "z", split_axis=0, concat_axis=0, tiled=True
    )
    other_rows = jnp.transpose(other_terms, (1, 0, 2))
    row_energy = lax.dynamic_slice_in_dim(virt_energy, lax.axis_index(XY) * ROW, ROW, 0)
    low_energy = (row_energy[:, None] - pair_energy[None, :]).reshape(ROW * PAIRS, 1)
    chunk = make_chunk(place, l_parts, other_rows, virt_energy[None, :], low_energy)
    l_mine = lax.all_gather(chunk, "z", axis=0, tiled=True)
    l_rest = core_swap(l_mine)

    marks = jnp.concatenate([l_mine, l_rest]).reshape(NC * NZ, CHUNK * PAIRS, WIDE)
    squares = jnp.sum(marks[:, 0, NVIR : NVIR + 3].astype(F32))
    total = jnp.broadcast_to(squares, (NV, 8, LANE))
    totals = lax.all_to_all(total, XY, split_axis=0, concat_axis=0, tiled=True)
    residual = jnp.transpose(make_final(place, l_mine, l_rest, other_rows), (1, 0, 2))
    count = PAIRS * NVIR * NVIR
    update_rms = jnp.sqrt(jnp.sum(totals[:, 0, 0]) / count + epsilon)
    return residual, update_rms


def solution(mesh):
    torus = Mesh(mesh.devices.reshape(NX, NY, NZ, NC), AXES)
    return jax.shard_map(
        shards,
        mesh=torus,
        in_specs=(
            P(None, XY, RANK),
            P(XY, RANK),
            P(XY, RANK),
            P(None, XY, None),
            P(),
            P(),
        ),
        out_specs=(P(None, XY, None), P()),
        check_vma=False,
    )
```

```python
import jax
import jax.numpy as jnp
from jax import lax
from jax.experimental import pallas as pl
from jax.experimental.pallas import tpu as pltpu
from jax.sharding import Mesh
from jax.sharding import PartitionSpec as P

AXES = ("x", "y", "z", "c")
XY = ("x", "y")
RANK = ("z", "c")
BF = jnp.bfloat16
F32 = jnp.float32
epsilon = 1e-06

NX, NY, NZ, NC = 4, 4, 8, 2
NV = NX * NY
PAIRS = 8
ROW = 75
PAD = 80
BLK = 512
QC = 32
NVIR = 1200
LANE = 128
HALF = PAD // 2
CHUNK = 5
WIDE = 1280


def core_swap(value):
    return lax.ppermute(value, "c", [(0, 1), (1, 0)])


def ring(shift):
    return [(s, (s + shift) % NZ) for s in range(NZ)]


def regroup(tiles, want):
    out = None
    lane = lax.broadcasted_iota(jnp.int32, (PAD, LANE), 1) // QC
    for group, tile in enumerate(tiles):
        shift = ((group - want) * QC) % LANE
        moved = pltpu.roll(tile, shift, 1) if shift else tile
        out = moved if out is None else jnp.where(lane == group, moved, out)
    return out


def half_kernel(core_ref, own_ref, oth_ref, xz_ref, out_ref, acc_ref):
    core = core_ref[0]
    dims = (((0,), (0,)), ((), ()))
    x_own = xz_ref[:, core, :PAD, :].reshape(NZ * PAD, BLK)
    x_oth = xz_ref[:, 1 - core, :PAD, :].reshape(NZ * PAD, BLK)
    acc_ref[...] = lax.dot_general(
        own_ref[...], x_own, dims, preferred_element_type=F32
    ) + lax.dot_general(oth_ref[...], x_oth, dims, preferred_element_type=F32)
    for xx in range(NX):
        for half in range(2):
            tiles = [
                acc_ref[pl.ds((half * 4 + g) * PAD, PAD), pl.ds(xx * LANE, LANE)]
                for g in range(4)
            ]
            for yy in range(NY):
                out_ref[xx * NY + yy, :, pl.ds(half * LANE, LANE)] = regroup(tiles, yy).astype(BF)


def make_half(place, t_own, t_oth, xz):
    return pl.pallas_call(
        half_kernel,
        out_shape=jax.ShapeDtypeStruct((NV, PAD, PAIRS * QC), BF),
        in_specs=[pl.BlockSpec(memory_space=pltpu.SMEM)]
        + [pl.BlockSpec(memory_space=pltpu.VMEM)] * 3,
        scratch_shapes=[pltpu.VMEM((PAIRS * PAD, BLK), F32)],
        name="half",
    )(place, t_own, t_oth, xz)


FIRST = (0, 1, NZ - 1, 3, 4, 5)
LAST = (2, NZ - 2)
HALF_M = PAIRS * QC


def back_block(h, x, z_own, z_oth):
    coupled = jnp.dot(h, x, preferred_element_type=F32)
    z_own = z_own.reshape(1, QC, BLK).astype(F32)
    z_oth = z_oth.reshape(1, QC, BLK).astype(F32)
    c_own = coupled[:HALF_M].reshape(PAIRS, QC, BLK) * z_own
    c_oth = coupled[HALF_M:].reshape(PAIRS, QC, BLK) * z_oth
    w = jnp.concatenate(
        [c_own.reshape(HALF_M, BLK), c_oth.reshape(HALF_M, BLK)], axis=0
    ).astype(BF)
    return lax.dot_general(x, w, (((1,), (1,)), ((), ())), preferred_element_type=F32)


def first_kernel(
    place_ref, ho_ref, hx_ref, xq_ref, xu_ref, xd_ref, x_ref, zo_ref, zx_ref, acc_ref, h_ref, now_ref
):
    step = pl.program_id(0)

    @pl.when(step == 0)
    def _():
        h_ref[pl.ds(0, HALF_M), :] = ho_ref[...].astype(F32).T.astype(BF)
        h_ref[pl.ds(HALF_M, HALF_M), :] = hx_ref[...].astype(F32).T.astype(BF)
        acc_ref[...] = jnp.zeros_like(acc_ref)
        now_ref[...] = xq_ref[:, :PAD, :].reshape(NV * PAD, BLK)

    @pl.when(step == 1)
    def _():
        now_ref[...] = xu_ref[...].reshape(NV * PAD, BLK)

    @pl.when(step == 2)
    def _():
        now_ref[...] = xd_ref[...].reshape(NV * PAD, BLK)

    @pl.when(step > 2)
    def _():
        now_ref[...] = x_ref[...].reshape(NV * PAD, BLK)

    acc_ref[...] += back_block(h_ref[...], now_ref[...], zo_ref[0, 0, PAD:, :], zx_ref[...])


def first_level(step, place):
    far = jnp.where(step == 2, NZ - 1, step)
    return (place[1] + far) % NZ


def make_first(place, h_own, h_oth, xz, x_up, x_down, x_all, z_oth):
    rows = NV * PAD
    whole = pl.BlockSpec((NV, PAD, BLK), lambda k, p: (0, 0, 0))
    return pl.pallas_call(
        first_kernel,
        out_shape=(
            jax.ShapeDtypeStruct((rows, 2 * HALF_M), F32),
            jax.ShapeDtypeStruct((2 * HALF_M, rows), BF),
        ),
        grid_spec=pltpu.PrefetchScalarGridSpec(
            num_scalar_prefetch=1,
            grid=(len(FIRST),),
            in_specs=[
                pl.BlockSpec((rows, HALF_M), lambda k, p: (0, 0)),
                pl.BlockSpec((rows, HALF_M), lambda k, p: (0, 0)),
                pl.BlockSpec((NV, PAD + QC, BLK), lambda k, p: (0, 0, 0)),
                whole,
                whole,
                pl.BlockSpec((NV, 1, PAD, BLK), lambda k, p: (0, jnp.maximum(k - 3, 0), 0, 0)),
                pl.BlockSpec((1, 1, PAD + QC, BLK), lambda k, p: (first_level(k, p), p[0], 0, 0)),
                pl.BlockSpec((1, QC, BLK), lambda k, p: (first_level(k, p), 0, 0)),
            ],
            out_specs=(
                pl.BlockSpec((rows, 2 * HALF_M), lambda k, p: (0, 0)),
                pl.BlockSpec((2 * HALF_M, rows), lambda k, p: (0, 0)),
            ),
            scratch_shapes=[pltpu.VMEM((rows, BLK), BF)],
        ),
        compiler_params=pltpu.CompilerParams(dimension_semantics=("arbitrary",)),
        cost_estimate=pl.CostEstimate(
            flops=4 * 512 * 1280 * 512 * len(FIRST), bytes_accessed=12_000_000, transcendentals=0
        ),
        name="core_first",
    )(place, h_own, h_oth, xz, x_up, x_down, x_all, xz.reshape(NZ, NC, PAD + QC, BLK), z_oth)


def last_kernel(
    place_ref, acc_ref, h_ref, xu_ref, xd_ref, zou_ref, zxu_ref, zod_ref, zxd_ref, bo_ref, bx_ref
):
    h = h_ref[...]
    up = xu_ref[...].reshape(NV * PAD, BLK)
    down = xd_ref[...].reshape(NV * PAD, BLK)
    total = acc_ref[...] + back_block(h, up, zou_ref[0, 0, PAD:, :], zxu_ref[...])
    total += back_block(h, down, zod_ref[0, 0, PAD:, :], zxd_ref[...])
    bo_ref[...] = total[:, :HALF_M]
    bx_ref[...] = total[:, HALF_M:].astype(BF)


def make_last(place, acc, h, x_up, x_down, xz, z_oth):
    rows = NV * PAD
    whole = pl.BlockSpec((NV, PAD, BLK), lambda k, p: (0, 0, 0))

    def z_specs(far):
        return [
            pl.BlockSpec((1, 1, PAD + QC, BLK), lambda k, p: ((p[1] + far) % NZ, p[0], 0, 0)),
            pl.BlockSpec((1, QC, BLK), lambda k, p: ((p[1] + far) % NZ, 0, 0)),
        ]

    z_all = xz.reshape(NZ, NC, PAD + QC, BLK)
    return pl.pallas_call(
        last_kernel,
        out_shape=(
            jax.ShapeDtypeStruct((rows, HALF_M), F32),
            jax.ShapeDtypeStruct((rows, HALF_M), BF),
        ),
        grid_spec=pltpu.PrefetchScalarGridSpec(
            num_scalar_prefetch=1,
            grid=(1,),
            in_specs=[
                pl.BlockSpec((rows, 2 * HALF_M), lambda k, p: (0, 0)),
                pl.BlockSpec((2 * HALF_M, rows), lambda k, p: (0, 0)),
                whole,
                whole,
            ]
            + z_specs(LAST[0])
            + z_specs(LAST[1]),
            out_specs=(
                pl.BlockSpec((rows, HALF_M), lambda k, p: (0, 0)),
                pl.BlockSpec((rows, HALF_M), lambda k, p: (0, 0)),
            ),
        ),
        compiler_params=pltpu.CompilerParams(dimension_semantics=("arbitrary",)),
        cost_estimate=pl.CostEstimate(
            flops=4 * 512 * 1280 * 512 * len(LAST), bytes_accessed=8_000_000, transcendentals=0
        ),
        name="core_last",
    )(place, acc, h, x_up, x_down, z_all, z_oth, z_all, z_oth)


def ladder_kernel(place_ref, b_ref, x_ref, own_ref, oth_ref, g_ref):
    core = place_ref[0]
    for xx in range(NX):
        for half in range(2):
            tiles = [
                b_ref[xx * NY + yy, :, pl.ds(half * LANE, LANE)].astype(F32) for yy in range(NY)
            ]
            for g in range(4):
                g_ref[xx, pl.ds(half * 4 + g, PAD, stride=PAIRS), :] = regroup(tiles, g)
    dims = (((1,), (1,)), ((), ()))
    rows = HALF * PAIRS

    def gathered(which):
        start = pl.multiple_of(which * rows, rows)
        return jnp.concatenate([g_ref[xx, pl.ds(start, rows), :] for xx in range(NX)], axis=1)

    own = gathered(core).astype(BF)
    oth = gathered(1 - core).astype(BF)
    own_ref[...] = lax.dot_general(own, x_ref[...], dims, preferred_element_type=F32)
    oth_ref[...] = lax.dot_general(oth, x_ref[...], dims, preferred_element_type=F32).astype(BF)


def make_ladder(place, b_all, x_rows):
    return pl.pallas_call(
        ladder_kernel,
        out_shape=(
            jax.ShapeDtypeStruct((HALF * PAIRS, NVIR), F32),
            jax.ShapeDtypeStruct((HALF * PAIRS, NVIR), BF),
        ),
        in_specs=[pl.BlockSpec(memory_space=pltpu.SMEM)]
        + [pl.BlockSpec(memory_space=pltpu.VMEM)] * 2,
        scratch_shapes=[pltpu.VMEM((NX, PAIRS * PAD, LANE), F32)],
        name="ladder_rank",
    )(place, b_all, x_rows)


def chunk_kernel(place_ref, parts_ref, other_ref, col_ref, low_ref, out_ref):
    total = jnp.sum(parts_ref[...].astype(F32), axis=0)
    res = total + other_ref[...].reshape(CHUNK * PAIRS, NVIR)
    upd = res / (low_ref[...] + col_ref[...])
    squares = jnp.sum(upd * upd, axis=1, keepdims=True)
    squares = jnp.sum(squares, axis=0, keepdims=True)
    real = NC * NZ - 1
    squares = jnp.where(place_ref[2] < real, squares, 0.0)
    high = squares.astype(BF)
    rest = squares - high.astype(F32)
    mid = rest.astype(BF)
    low = (rest - mid.astype(F32)).astype(BF)
    out_ref[:, :NVIR] = total.astype(BF)
    lanes = WIDE - NVIR
    lane = lax.broadcasted_iota(jnp.int32, (CHUNK * PAIRS, lanes), 1)
    row = lax.broadcasted_iota(jnp.int32, (CHUNK * PAIRS, lanes), 0)
    kept = jnp.where(
        lane == 0, high.astype(F32), jnp.where(lane == 1, mid.astype(F32), low.astype(F32))
    )
    kept = jnp.where((row == 0) & (lane < 3), kept, 0.0)
    out_ref[:, NVIR:] = kept.astype(BF)


def make_chunk(place, parts, other_rows, col_energy, low_energy):
    last = ROW // CHUNK - 1
    return pl.pallas_call(
        chunk_kernel,
        out_shape=jax.ShapeDtypeStruct((CHUNK * PAIRS, WIDE), BF),
        grid_spec=pltpu.PrefetchScalarGridSpec(
            num_scalar_prefetch=1,
            grid=(1,),
            in_specs=[
                pl.BlockSpec((NZ, CHUNK * PAIRS, NVIR), lambda k, p: (0, 0, 0)),
                pl.BlockSpec((CHUNK, PAIRS, NVIR), lambda k, p: (jnp.minimum(p[2], last), 0, 0)),
                pl.BlockSpec((1, NVIR), lambda k, p: (0, 0)),
                pl.BlockSpec((CHUNK * PAIRS, 1), lambda k, p: (jnp.minimum(p[2], last), 0)),
            ],
            out_specs=pl.BlockSpec((CHUNK * PAIRS, WIDE), lambda k, p: (0, 0)),
        ),
        name="chunk",
    )(place, parts, other_rows, col_energy, low_energy)


def final_kernel(place_ref, own_ref, oth_ref, other_ref, out_ref):
    def fill(first, second):
        top = first[:, :NVIR].astype(F32).reshape(HALF, PAIRS, NVIR)
        out_ref[:HALF] = other_ref[:HALF] + top
        left = ROW - HALF
        end = second[: left * PAIRS, :NVIR].astype(F32).reshape(left, PAIRS, NVIR)
        out_ref[HALF:] = other_ref[HALF:] + end

    @pl.when(place_ref[0] == 0)
    def _():
        fill(own_ref, oth_ref)

    @pl.when(place_ref[0] == 1)
    def _():
        fill(oth_ref, own_ref)


def make_final(place, l_own, l_oth, other_rows):
    return pl.pallas_call(
        final_kernel,
        out_shape=jax.ShapeDtypeStruct((ROW, PAIRS, NVIR), F32),
        in_specs=[pl.BlockSpec(memory_space=pltpu.SMEM)]
        + [pl.BlockSpec(memory_space=pltpu.VMEM)] * 3,
        name="residual",
    )(place, l_own, l_oth, other_rows)


def shards(amplitudes, factors, kernel, other_terms, virt_energy, pair_energy):
    core = lax.axis_index("c").astype(jnp.int32)
    level = lax.axis_index("z").astype(jnp.int32)
    place = jnp.stack([core, level, core * NZ + level])

    x_pad = jnp.pad(factors, ((0, PAD - ROW), (0, 0)))
    z_cols = kernel.T.reshape(NV, QC, BLK)
    xz = jnp.concatenate([jnp.broadcast_to(x_pad[None], (NV, PAD, BLK)), z_cols], axis=1)
    x_pad, xz = lax.optimization_barrier((x_pad, xz))
    xz = lax.all_to_all(xz, XY, split_axis=0, concat_axis=0, tiled=True)
    x_far = jnp.stack([lax.ppermute(x_pad, "z", ring(-j)) for j in FIRST[3:]])
    x_all = lax.all_to_all(
        jnp.broadcast_to(x_far[None], (NV, *x_far.shape)),
        XY,
        split_axis=0,
        concat_axis=0,
        tiled=True,
    )

    t_cols = jnp.pad(amplitudes, ((0, 0), (0, PAD - ROW), (0, PAD - ROW)))
    t_cols = jnp.transpose(t_cols, (2, 0, 1)).reshape(PAD, PAIRS * PAD)
    t_cols, _, _ = lax.optimization_barrier((t_cols, x_far, xz))
    t_own = lax.all_gather(t_cols, "z", axis=0, tiled=True)
    t_oth = core_swap(t_own)
    x_own = xz[:, :PAD]
    x_up = lax.ppermute(x_own, "z", ring(-1))
    x_down = lax.ppermute(x_own, "z", ring(1))
    x_up2 = lax.ppermute(x_up, "z", ring(-1))
    x_down2 = lax.ppermute(x_down, "z", ring(1))
    x_rows = xz[:, :ROW].reshape(NVIR, BLK)

    t_own, t_oth, _, _ = lax.optimization_barrier((t_own, t_oth, x_up, x_down))
    h_msg = make_half(place, t_own, t_oth, xz.reshape(NZ, NC, PAD + QC, BLK))
    h_msg, x_all = lax.optimization_barrier((h_msg, x_all))
    h_own = lax.all_to_all(h_msg, XY, split_axis=0, concat_axis=0, tiled=True)
    h_own = h_own.reshape(NV * PAD, PAIRS * QC)
    h_oth = core_swap(h_own)
    z_all = xz.reshape(NZ, NC, PAD + QC, BLK)
    z_oth = lax.dynamic_index_in_dim(z_all, 1 - core, 1, keepdims=False)[:, PAD:]
    z_oth = core_swap(z_oth)

    acc, h = make_first(place, h_own, h_oth, xz, x_up, x_down, x_all, z_oth)
    b_own, b_send = make_last(place, acc, h, x_up2, x_down2, xz, z_oth)
    b_sum = (b_own + core_swap(b_send).astype(F32)).astype(BF)
    b_all = lax.all_to_all(
        b_sum.reshape(NV, PAD, PAIRS * QC), XY, split_axis=0, concat_axis=0, tiled=True
    )

    l_own, l_send = make_ladder(place, b_all, x_rows)
    l_sum = (l_own + core_swap(l_send).astype(F32)).astype(BF)
    l_parts = lax.all_to_all(
        l_sum.reshape(NZ, CHUNK * PAIRS, NVIR), "z", split_axis=0, concat_axis=0, tiled=True
    )
    other_rows = jnp.transpose(other_terms, (1, 0, 2))
    row_energy = lax.dynamic_slice_in_dim(virt_energy, lax.axis_index(XY) * ROW, ROW, 0)
    low_energy = (row_energy[:, None] - pair_energy[None, :]).reshape(ROW * PAIRS, 1)
    chunk = make_chunk(place, l_parts, other_rows, virt_energy[None, :], low_energy)
    l_mine = lax.all_gather(chunk, "z", axis=0, tiled=True)
    l_rest = core_swap(l_mine)

    marks = jnp.concatenate([l_mine, l_rest]).reshape(NC * NZ, CHUNK * PAIRS, WIDE)
    squares = jnp.sum(marks[:, 0, NVIR : NVIR + 3].astype(F32))
    total = jnp.broadcast_to(squares, (NV, 8, LANE))
    totals = lax.all_to_all(total, XY, split_axis=0, concat_axis=0, tiled=True)
    residual = jnp.transpose(make_final(place, l_mine, l_rest, other_rows), (1, 0, 2))
    count = PAIRS * NVIR * NVIR
    update_rms = jnp.sqrt(jnp.sum(totals[:, 0, 0]) / count + epsilon)
    return residual, update_rms


def solution(mesh):
    torus = Mesh(mesh.devices.reshape(NX, NY, NZ, NC), AXES)
    return jax.shard_map(
        shards,
        mesh=torus,
        in_specs=(
            P(None, XY, RANK),
            P(XY, RANK),
            P(XY, RANK),
            P(None, XY, None),
            P(),
            P(),
        ),
        out_specs=(P(None, XY, None), P()),
        check_vma=False,
    )
```

```python
import jax
import jax.numpy as jnp
from jax import lax
from jax.experimental import pallas as pl
from jax.experimental.pallas import tpu as pltpu
from jax.sharding import Mesh
from jax.sharding import PartitionSpec as P

AXES = ("x", "y", "z", "c")
XY = ("x", "y")
RANK = ("z", "c")
BF = jnp.bfloat16
F32 = jnp.float32
epsilon = 1e-06

NX, NY, NZ, NC = 4, 4, 8, 2
NV = NX * NY
PAIRS = 8
ROW = 75
PAD = 80
BLK = 512
QC = 32
NVIR = 1200
LANE = 128
HALF = PAD // 2
WIDE = 1280


def core_swap(value):
    return lax.ppermute(value, "c", [(0, 1), (1, 0)])


def ring(shift):
    return [(s, (s + shift) % NZ) for s in range(NZ)]


def regroup(tiles, want):
    out = None
    lane = lax.broadcasted_iota(jnp.int32, (PAD, LANE), 1) // QC
    for group, tile in enumerate(tiles):
        shift = ((group - want) * QC) % LANE
        moved = pltpu.roll(tile, shift, 1) if shift else tile
        out = moved if out is None else jnp.where(lane == group, moved, out)
    return out


ORDER = (0, 1, NZ - 1, 2, 3, 4, 5, 6)
NEAR = 3
HALF_M = PAIRS * QC


def level_of(step, place):
    far = jnp.where(step == 2, NZ - 1, jnp.where(step > 2, step - 1, step))
    return (place[1] + far) % NZ


def x_specs():
    whole = pl.BlockSpec((NV, PAD, BLK), lambda k, p: (0, 0, 0))
    return [
        pl.BlockSpec((NV, PAD + QC, BLK), lambda k, p: (0, 0, 0)),
        whole,
        whole,
        pl.BlockSpec((NV, 1, PAD, BLK), lambda k, p: (0, jnp.maximum(k - NEAR, 0), 0, 0)),
    ]


def with_block(step, xq_ref, xu_ref, xd_ref, x_ref, body):
    @pl.when(step == 0)
    def _():
        body(xq_ref[:, :PAD, :].reshape(NV * PAD, BLK))

    @pl.when(step == 1)
    def _():
        body(xu_ref[...].reshape(NV * PAD, BLK))

    @pl.when(step == 2)
    def _():
        body(xd_ref[...].reshape(NV * PAD, BLK))

    @pl.when(step > 2)
    def _():
        body(x_ref[...].reshape(NV * PAD, BLK))


def half_kernel(place_ref, to_ref, tx_ref, xq_ref, xu_ref, xd_ref, x_ref, out_ref, t_ref, tt_ref, acc_ref):
    step = pl.program_id(0)
    core, level = place_ref[0], place_ref[1]

    @pl.when(step == 0)
    def _():
        for j in range(NZ):
            rank = 2 * ((level + NZ - j) % NZ)
            own = pl.multiple_of((rank + core) * PAD, PAD)
            oth = pl.multiple_of((rank + 1 - core) * PAD, PAD)
            t_ref[pl.ds(own, PAD), :] = to_ref[j].astype(F32)
            t_ref[pl.ds(oth, PAD), :] = tx_ref[j].astype(F32)
        tt_ref[...] = t_ref[...].T.astype(BF)

    def body(x):
        acc_ref[level_of(step, place_ref)] = jnp.dot(
            tt_ref[...], x, preferred_element_type=F32
        )

    with_block(step, xq_ref, xu_ref, xd_ref, x_ref, body)

    @pl.when(step == NZ - 1)
    def _():
        for xx in range(NX):
            for half in range(2):
                tiles = [acc_ref[half * 4 + g, :, pl.ds(xx * LANE, LANE)] for g in range(4)]
                for yy in range(NY):
                    out_ref[xx * NY + yy, :, pl.ds(half * LANE, LANE)] = regroup(
                        tiles, yy
                    ).astype(BF)


def make_half(place, t_own, t_oth, xs):
    piece = pl.BlockSpec((NZ, PAD, PAD), lambda k, p: (0, 0, 0))
    return pl.pallas_call(
        half_kernel,
        out_shape=jax.ShapeDtypeStruct((NV, PAD, HALF_M), BF),
        grid_spec=pltpu.PrefetchScalarGridSpec(
            num_scalar_prefetch=1,
            grid=(NZ,),
            in_specs=[piece, piece] + x_specs(),
            out_specs=pl.BlockSpec((NV, PAD, HALF_M), lambda k, p: (0, 0, 0)),
            scratch_shapes=[
                pltpu.VMEM((NV * PAD, PAD), F32),
                pltpu.VMEM((PAD, NV * PAD), BF),
                pltpu.VMEM((NZ, PAD, BLK), F32),
            ],
        ),
        compiler_params=pltpu.CompilerParams(dimension_semantics=("arbitrary",)),
        name="half",
    )(place, t_own, t_oth, *xs)


def main_kernel(
    place_ref, ho_ref, hx_ref, xq_ref, xu_ref, xd_ref, x_ref, *rest
):
    pieces, (bo_ref, bx_ref, h_ref, z_ref, acc_ref) = rest[:-5], rest[-5:]
    step = pl.program_id(0)
    level = place_ref[1]

    @pl.when(step == 0)
    def _():
        h_ref[pl.ds(0, HALF_M), :] = ho_ref[...].astype(F32).T.astype(BF)
        h_ref[pl.ds(HALF_M, HALF_M), :] = hx_ref[...].astype(F32).T.astype(BF)
        acc_ref[...] = jnp.zeros_like(acc_ref)

    for (far, first, count), ref in zip(Z_PARTS, pieces):
        start = ((level + far) % NZ) * QC
        for j in range(count):
            at = pl.multiple_of((first + j) * HALF_M + start, QC)
            z_ref[pl.ds(at, QC), :] = ref[j, 0].astype(F32)

    def body(x):
        coupled = jnp.dot(h_ref[...], x, preferred_element_type=F32)
        w = (coupled * z_ref[...]).astype(BF)
        acc_ref[...] += lax.dot_general(
            x, w, (((1,), (1,)), ((), ())), preferred_element_type=F32
        )

    with_block(step, xq_ref, xu_ref, xd_ref, x_ref, body)

    @pl.when(step == NZ - 1)
    def _():
        bo_ref[...] = acc_ref[:, :HALF_M]
        bx_ref[...] = acc_ref[:, HALF_M:].astype(BF)


Z_PARTS = (
    (0, 0, 2),
    (1, 0, 2),
    (2, 0, 2),
    (3, 0, 2),
    (7, 0, 2),
    (6, 0, 2),
    (5, 0, 2),
    (4, 0, 1),
    (4, 1, 1),
)


def make_main(place, h_own, h_oth, xs, z_pieces):
    rows = NV * PAD

    def z_spec(count):
        return pl.BlockSpec((count, 1, QC, BLK), lambda k, p: (0, level_of(k, p), 0, 0))

    flat = pl.BlockSpec((rows, HALF_M), lambda k, p: (0, 0))
    return pl.pallas_call(
        main_kernel,
        out_shape=(
            jax.ShapeDtypeStruct((rows, HALF_M), F32),
            jax.ShapeDtypeStruct((rows, HALF_M), BF),
        ),
        grid_spec=pltpu.PrefetchScalarGridSpec(
            num_scalar_prefetch=1,
            grid=(NZ,),
            in_specs=[flat, flat] + x_specs() + [z_spec(part[2]) for part in Z_PARTS],
            out_specs=(flat, flat),
            scratch_shapes=[
                pltpu.VMEM((2 * HALF_M, rows), BF),
                pltpu.VMEM((2 * HALF_M, BLK), F32),
                pltpu.VMEM((rows, 2 * HALF_M), F32),
            ],
        ),
        compiler_params=pltpu.CompilerParams(dimension_semantics=("arbitrary",)),
        cost_estimate=pl.CostEstimate(
            flops=4 * 512 * 1280 * 4096, bytes_accessed=18_000_000, transcendentals=0
        ),
        name="core",
    )(place, h_own, h_oth, *xs, *z_pieces)


def ladder_kernel(
    place_ref, b_ref, xq_ref, xu_ref, xd_ref, x_ref, own_ref, oth_ref, g_ref, acc_ref
):
    step = pl.program_id(0)

    @pl.when(step == 0)
    def _():
        for xx in range(NX):
            for half in range(2):
                tiles = [
                    b_ref[xx * NY + yy, :, pl.ds(half * LANE, LANE)].astype(F32)
                    for yy in range(NY)
                ]
                for g in range(4):
                    g_ref[half * 4 + g, :, pl.ds(xx * LANE, LANE)] = regroup(tiles, g).astype(BF)
        acc_ref[...] = jnp.zeros_like(acc_ref)

    def body(x):
        acc_ref[...] += lax.dot_general(
            g_ref[level_of(step, place_ref)],
            x,
            (((1,), (1,)), ((), ())),
            preferred_element_type=F32,
        )

    with_block(step, xq_ref, xu_ref, xd_ref, x_ref, body)

    @pl.when(step == NZ - 1)
    def _():
        core = place_ref[0]
        own_ref[...] = acc_ref[pl.ds(pl.multiple_of(core * HALF, HALF), HALF), :]
        oth_ref[...] = acc_ref[pl.ds(pl.multiple_of((1 - core) * HALF, HALF), HALF), :]


def make_ladder(place, b_all, xs):
    flat = pl.BlockSpec((HALF, WIDE), lambda k, p: (0, 0))
    return pl.pallas_call(
        ladder_kernel,
        out_shape=(
            jax.ShapeDtypeStruct((HALF, WIDE), F32),
            jax.ShapeDtypeStruct((HALF, WIDE), F32),
        ),
        grid_spec=pltpu.PrefetchScalarGridSpec(
            num_scalar_prefetch=1,
            grid=(NZ,),
            in_specs=[pl.BlockSpec((NV, PAD, HALF_M), lambda k, p: (0, 0, 0))] + x_specs(),
            out_specs=(flat, flat),
            scratch_shapes=[
                pltpu.VMEM((NZ, PAD, BLK), BF),
                pltpu.VMEM((PAD, WIDE), F32),
            ],
        ),
        compiler_params=pltpu.CompilerParams(dimension_semantics=("arbitrary",)),
        name="ladder",
    )(place, b_all, *xs)


def chunk_kernel(place_ref, own_ref, oth_ref, other_ref, col_ref, low_ref, out_ref):
    wide = own_ref[...] + oth_ref[...]
    lane = lax.broadcasted_iota(jnp.int32, (HALF, WIDE), 1)
    row = lax.broadcasted_iota(jnp.int32, (HALF, WIDE), 0)
    total = wide
    for v in range(1, NV):
        moved = pltpu.roll(wide, WIDE - v * (PAD - ROW), 1)
        total = jnp.where(lane >= v * ROW, moved, total)
    res = total[:, :NVIR] + other_ref[...]
    upd = res / (low_ref[...] + col_ref[...])
    real = row[:, :NVIR] + place_ref[0] * HALF < ROW
    upd = jnp.where(real, upd, 0.0)
    squares = jnp.sum(upd * upd, axis=1, keepdims=True)
    squares = jnp.sum(squares, axis=0, keepdims=True)
    high = squares.astype(BF).astype(F32)
    rest = squares - high
    mid = rest.astype(BF).astype(F32)
    low = rest - mid
    kept = jnp.where(lane == NVIR, high, jnp.where(lane == NVIR + 1, mid, low))
    kept = jnp.where((row == 0) & (lane < NVIR + 3), kept, 0.0)
    out_ref[...] = jnp.where(lane < NVIR, total, kept).astype(BF)


def make_chunk(place, own, oth, other_part, col_energy, low_energy):
    return pl.pallas_call(
        chunk_kernel,
        out_shape=jax.ShapeDtypeStruct((HALF, WIDE), BF),
        in_specs=[pl.BlockSpec(memory_space=pltpu.SMEM)]
        + [pl.BlockSpec(memory_space=pltpu.VMEM)] * 5,
        name="chunk",
    )(place, own, oth, other_part, col_energy, low_energy)


def final_kernel(place_ref, own_ref, oth_ref, other_ref, out_ref, mix_ref):
    def fill(source, start, count):
        for t in range(WIDE // LANE):
            lanes = min(LANE, NVIR - t * LANE)
            for i in range(PAIRS):
                mix_ref[t, pl.ds(i, HALF, stride=PAIRS), :] = source[
                    i, :, pl.ds(t * LANE, LANE)
                ].astype(F32)
            part = mix_ref[t, : count * PAIRS, :lanes].reshape(count, PAIRS, lanes)
            at = (pl.ds(start, count), slice(None), pl.ds(t * LANE, lanes))
            out_ref[at] = other_ref[at] + part

    @pl.when(place_ref[0] == 0)
    def _():
        fill(own_ref, 0, HALF)
        fill(oth_ref, HALF, ROW - HALF)

    @pl.when(place_ref[0] == 1)
    def _():
        fill(oth_ref, 0, HALF)
        fill(own_ref, HALF, ROW - HALF)


def make_final(place, l_own, l_oth, other_rows):
    return pl.pallas_call(
        final_kernel,
        out_shape=jax.ShapeDtypeStruct((ROW, PAIRS, NVIR), F32),
        in_specs=[pl.BlockSpec(memory_space=pltpu.SMEM)]
        + [pl.BlockSpec(memory_space=pltpu.VMEM)] * 3,
        scratch_shapes=[pltpu.VMEM((WIDE // LANE, HALF * PAIRS, LANE), F32)],
        name="residual",
    )(place, l_own, l_oth, other_rows)


def shards(amplitudes, factors, kernel, other_terms, virt_energy, pair_energy):
    core = lax.axis_index("c").astype(jnp.int32)
    level = lax.axis_index("z").astype(jnp.int32)
    place = jnp.stack([core, level])

    x_pad = jnp.pad(factors, ((0, PAD - ROW), (0, 0)))
    z_cols = kernel.T.reshape(NV, QC, BLK)
    xz = jnp.concatenate([jnp.broadcast_to(x_pad[None], (NV, PAD, BLK)), z_cols], axis=1)
    x_pad, xz = lax.optimization_barrier((x_pad, xz))
    xz = lax.all_to_all(xz, XY, split_axis=0, concat_axis=0, tiled=True)
    x_far = jnp.stack([lax.ppermute(x_pad, "z", ring(-j)) for j in ORDER[NEAR:]])
    x_all = lax.all_to_all(
        jnp.broadcast_to(x_far[None], (NV, *x_far.shape)),
        XY,
        split_axis=0,
        concat_axis=0,
        tiled=True,
    )
    x_own = xz[:, :PAD]
    x_up = lax.ppermute(x_own, "z", ring(-1))
    x_down = lax.ppermute(x_own, "z", ring(1))
    xs = (xz, x_up, x_down, x_all)

    z_all = xz.reshape(NZ, NC, PAD + QC, BLK)
    z_own = lax.dynamic_index_in_dim(z_all, core, 1, keepdims=False)[:, PAD:]
    z_oth = lax.dynamic_index_in_dim(z_all, 1 - core, 1, keepdims=False)[:, PAD:]
    z_here = jnp.stack([z_own, core_swap(z_oth)])
    ups, downs = [z_here], [z_here]
    for _ in range(3):
        ups.append(lax.ppermute(ups[-1], "z", ring(-1)))
        downs.append(lax.ppermute(downs[-1], "z", ring(1)))
    last_up = lax.ppermute(ups[-1][:1], "z", ring(-1))
    last_down = lax.ppermute(downs[-1][1:], "z", ring(1))
    z_pieces = (*ups, *downs[1:], last_up, last_down)

    t_cols = jnp.pad(amplitudes, ((0, 0), (0, PAD - ROW), (0, PAD - ROW)))
    t_cols = jnp.transpose(t_cols, (0, 2, 1))
    t_cols = lax.dynamic_slice_in_dim(jnp.concatenate([t_cols, t_cols]), level, NZ, 0)
    t_own = jnp.stack(
        [t_cols[0]] + [lax.ppermute(t_cols[j], "z", ring(j)) for j in range(1, NZ)]
    )
    t_oth = core_swap(t_own)

    h_msg = make_half(place, t_own, t_oth, xs)
    h_own = lax.all_to_all(h_msg, XY, split_axis=0, concat_axis=0, tiled=True)
    h_own = h_own.reshape(NV * PAD, HALF_M)
    h_oth = core_swap(h_own)

    b_own, b_send = make_main(place, h_own, h_oth, xs, z_pieces)
    b_sum = (b_own + core_swap(b_send).astype(F32)).astype(BF)
    b_all = lax.all_to_all(
        b_sum.reshape(NV, PAD, HALF_M), XY, split_axis=0, concat_axis=0, tiled=True
    )

    l_own, l_send = make_ladder(place, b_all, xs)
    l_recv = core_swap(l_send)
    other_part = lax.dynamic_index_in_dim(other_terms, level, 0, keepdims=False)
    other_part = jnp.pad(other_part, ((0, PAD - ROW), (0, 0)))
    other_part = lax.dynamic_slice_in_dim(other_part, core * HALF, HALF, 0)
    row_energy = lax.dynamic_slice_in_dim(virt_energy, lax.axis_index(XY) * ROW, ROW, 0)
    low_energy = jnp.pad(row_energy, (0, PAD - ROW), constant_values=1.0)
    low_energy = lax.dynamic_slice_in_dim(low_energy, core * HALF, HALF, 0)
    low_energy = (low_energy - lax.dynamic_index_in_dim(pair_energy, level, 0))[:, None]
    chunk = make_chunk(place, l_own, l_recv, other_part, virt_energy[None, :], low_energy)
    l_mine = lax.all_gather(chunk, "z", axis=0)
    l_rest = core_swap(l_mine)

    marks = jnp.concatenate([l_mine, l_rest])
    squares = jnp.sum(marks[:, 0, NVIR : NVIR + 3].astype(F32))
    total = jnp.broadcast_to(squares, (NV, 8, LANE))
    totals = lax.all_to_all(total, XY, split_axis=0, concat_axis=0, tiled=True)
    other_rows = jnp.transpose(other_terms, (1, 0, 2))
    residual = jnp.transpose(make_final(place, l_mine, l_rest, other_rows), (1, 0, 2))
    count = PAIRS * NVIR * NVIR
    update_rms = jnp.sqrt(jnp.sum(totals[:, 0, 0]) / count + epsilon)
    return residual, update_rms


def solution(mesh):
    torus = Mesh(mesh.devices.reshape(NX, NY, NZ, NC), AXES)
    return jax.shard_map(
        shards,
        mesh=torus,
        in_specs=(
            P(None, XY, RANK),
            P(XY, RANK),
            P(XY, RANK),
            P(None, XY, None),
            P(),
            P(),
        ),
        out_specs=(P(None, XY, None), P()),
        check_vma=False,
    )
```

```python
import jax
import jax.numpy as jnp
from jax import lax
from jax.experimental import pallas as pl
from jax.experimental.pallas import tpu as pltpu
from jax.sharding import Mesh
from jax.sharding import PartitionSpec as P

AXES = ("x", "y", "z", "c")
XY = ("x", "y")
RANK = ("z", "c")
BF = jnp.bfloat16
F32 = jnp.float32
epsilon = 1e-06

NX, NY, NZ, NC = 4, 4, 8, 2
NV = NX * NY
PAIRS = 8
ROW = 75
PAD = 80
BLK = 512
QC = 32
NVIR = 1200
LANE = 128
HALF = PAD // 2
WIDE = 1280


def core_swap(value):
    return lax.ppermute(value, "c", [(0, 1), (1, 0)])


def ring(shift):
    return [(s, (s + shift) % NZ) for s in range(NZ)]


def around(value, first, second):
    def step(piece, axis, shift):
        return lax.ppermute(piece, axis, [(s, (s + shift) % 4) for s in range(4)])

    left, right = step(value, first, 1), step(value, first, -1)
    cut = BLK // 2
    across = jnp.concatenate(
        [step(left[..., :cut], first, 1), step(right[..., cut:], first, -1)], axis=-1
    )
    line = jnp.stack([value, left, right, across])
    left, right = step(line, second, 1), step(line, second, -1)
    return line, left, right, step(left[:2], second, 1), step(right[2:], second, -1)


def regroup(tiles, want):
    out = None
    lane = lax.broadcasted_iota(jnp.int32, (PAD, LANE), 1) // QC
    for group, tile in enumerate(tiles):
        shift = ((group - want) * QC) % LANE
        moved = pltpu.roll(tile, shift, 1) if shift else tile
        out = moved if out is None else jnp.where(lane == group, moved, out)
    return out


NEAR = 3
A_FAR = (2, 3, 4)
B_FAR = (5, 6)
SHIFTS = (0, -1, 1, 2)
HALF_M = PAIRS * QC


def level_of(step, place):
    far = jnp.where(step == 2, NZ - 1, jnp.where(step > 2, step - 1, step))
    return (place[1] + far) % NZ


def x_specs():
    whole = pl.BlockSpec((NV, PAD, BLK), lambda k, p: (0, 0, 0))

    def far(first, blocks, count):
        return pl.BlockSpec(
            (count, 1, PAD, BLK), lambda k, p: (0, jnp.clip(k - first, 0, blocks - 1), 0, 0)
        )

    a_specs = [far(NEAR, len(A_FAR), n) for n in (4, 4, 4, 2, 2)]
    b_specs = [far(NEAR + len(A_FAR), len(B_FAR), n) for n in (4, 4, 4, 2, 2)]
    return [pl.BlockSpec((NV, PAD + QC, BLK), lambda k, p: (0, 0, 0)), whole, whole, *a_specs, *b_specs]


X_REFS = 13
NOW = pltpu.VMEM((NV * PAD, BLK), BF)


def with_block(step, place, x_refs, now_ref, body):
    xq_ref, xu_ref, xd_ref = x_refs[:3]

    def place_rows(refs, swapped):
        parts = ((refs[0], 0, 0), (refs[1], -1, 0), (refs[2], 1, 0), (refs[3], 2, 0), (refs[4], 2, 2))
        for ref, outer, first in parts:
            for n in range(ref.shape[0]):
                inner = SHIFTS[first + n]
                dx, dy = (outer, inner) if swapped else (inner, outer)
                xx = (place[2] + (dx + NX)) % NX
                yy = (place[3] + (dy + NY)) % NY
                at = pl.multiple_of((xx * NY + yy) * PAD, PAD)
                now_ref[pl.ds(at, PAD), :] = ref[n, 0]

    @pl.when(step == 0)
    def _():
        now_ref[...] = xq_ref[:, :PAD, :].reshape(NV * PAD, BLK)

    @pl.when(step == 1)
    def _():
        now_ref[...] = xu_ref[...].reshape(NV * PAD, BLK)

    @pl.when(step == 2)
    def _():
        now_ref[...] = xd_ref[...].reshape(NV * PAD, BLK)

    @pl.when((step >= NEAR) & (step < NEAR + len(A_FAR)))
    def _():
        place_rows(x_refs[3:8], False)

    @pl.when(step >= NEAR + len(A_FAR))
    def _():
        place_rows(x_refs[8:13], True)

    body(now_ref[...])


def half_kernel(place_ref, to_ref, tx_ref, *rest):
    x_refs, (out_ref, t_ref, tt_ref, acc_ref, now_ref) = rest[:X_REFS], rest[X_REFS:]
    step = pl.program_id(0)
    core, level = place_ref[0], place_ref[1]

    @pl.when(step == 0)
    def _():
        for j in range(NZ):
            rank = 2 * ((level + j) % NZ)
            own = pl.multiple_of((rank + core) * PAD, PAD)
            oth = pl.multiple_of((rank + 1 - core) * PAD, PAD)
            t_ref[pl.ds(own, PAD), :] = to_ref[j].astype(F32).T[:PAD]
            t_ref[pl.ds(oth, PAD), :] = tx_ref[j].astype(F32).T[:PAD]
        tt_ref[...] = t_ref[...].T.astype(BF)

    def body(x):
        acc_ref[level_of(step, place_ref)] = jnp.dot(
            tt_ref[...], x, preferred_element_type=F32
        )

    with_block(step, place_ref, x_refs, now_ref, body)

    @pl.when(step == NZ - 1)
    def _():
        for xx in range(NX):
            for half in range(2):
                tiles = [acc_ref[half * 4 + g, :, pl.ds(xx * LANE, LANE)] for g in range(4)]
                for yy in range(NY):
                    out_ref[xx * NY + yy, :, pl.ds(half * LANE, LANE)] = regroup(
                        tiles, yy
                    ).astype(BF)


def make_half(place, t_own, t_oth, xs):
    piece = pl.BlockSpec((NZ, PAD, LANE), lambda k, p: (0, 0, 0))
    return pl.pallas_call(
        half_kernel,
        out_shape=jax.ShapeDtypeStruct((NV, PAD, HALF_M), BF),
        grid_spec=pltpu.PrefetchScalarGridSpec(
            num_scalar_prefetch=1,
            grid=(NZ,),
            in_specs=[piece, piece] + x_specs(),
            out_specs=pl.BlockSpec((NV, PAD, HALF_M), lambda k, p: (0, 0, 0)),
            scratch_shapes=[
                pltpu.VMEM((NV * PAD, PAD), F32),
                pltpu.VMEM((PAD, NV * PAD), BF),
                pltpu.VMEM((NZ, PAD, BLK), F32),
                NOW,
            ],
        ),
        compiler_params=pltpu.CompilerParams(dimension_semantics=("arbitrary",)),
        name="half",
    )(place, t_own, t_oth, *xs)


def main_kernel(place_ref, ho_ref, hx_ref, *rest):
    x_refs, rest = rest[:X_REFS], rest[X_REFS:]
    pieces, (bo_ref, bx_ref, h_ref, z_ref, acc_ref, now_ref) = rest[:-6], rest[-6:]
    step = pl.program_id(0)
    level = place_ref[1]

    @pl.when(step == 0)
    def _():
        h_ref[pl.ds(0, HALF_M), :] = ho_ref[...].astype(F32).T.astype(BF)
        h_ref[pl.ds(HALF_M, HALF_M), :] = hx_ref[...].astype(F32).T.astype(BF)
        acc_ref[...] = jnp.zeros_like(acc_ref)

    for (far, first, count), ref in zip(Z_PARTS, pieces):
        start = ((level + far) % NZ) * QC
        for j in range(count):
            at = pl.multiple_of((first + j) * HALF_M + start, QC)
            z_ref[pl.ds(at, QC), :] = ref[j, 0].astype(F32)

    def body(x):
        coupled = jnp.dot(h_ref[...], x, preferred_element_type=F32)
        w = (coupled * z_ref[...]).astype(BF)
        acc_ref[...] += lax.dot_general(
            x, w, (((1,), (1,)), ((), ())), preferred_element_type=F32
        )

    with_block(step, place_ref, x_refs, now_ref, body)

    @pl.when(step == NZ - 1)
    def _():
        bo_ref[...] = acc_ref[:, :HALF_M]
        bx_ref[...] = acc_ref[:, HALF_M:].astype(BF)


Z_PARTS = (
    (0, 0, 2),
    (1, 0, 2),
    (2, 0, 2),
    (3, 0, 2),
    (7, 0, 2),
    (6, 0, 2),
    (5, 0, 2),
    (4, 0, 1),
    (4, 1, 1),
)


def make_main(place, h_own, h_oth, xs, z_pieces):
    rows = NV * PAD

    def z_spec(count):
        return pl.BlockSpec((count, 1, QC, BLK), lambda k, p: (0, level_of(k, p), 0, 0))

    flat = pl.BlockSpec((rows, HALF_M), lambda k, p: (0, 0))
    return pl.pallas_call(
        main_kernel,
        out_shape=(
            jax.ShapeDtypeStruct((rows, HALF_M), F32),
            jax.ShapeDtypeStruct((rows, HALF_M), BF),
        ),
        grid_spec=pltpu.PrefetchScalarGridSpec(
            num_scalar_prefetch=1,
            grid=(NZ,),
            in_specs=[flat, flat] + x_specs() + [z_spec(part[2]) for part in Z_PARTS],
            out_specs=(flat, flat),
            scratch_shapes=[
                pltpu.VMEM((2 * HALF_M, rows), BF),
                pltpu.VMEM((2 * HALF_M, BLK), F32),
                pltpu.VMEM((rows, 2 * HALF_M), F32),
                NOW,
            ],
        ),
        compiler_params=pltpu.CompilerParams(dimension_semantics=("arbitrary",)),
        cost_estimate=pl.CostEstimate(
            flops=4 * 512 * 1280 * 4096, bytes_accessed=18_000_000, transcendentals=0
        ),
        name="core",
    )(place, h_own, h_oth, *xs, *z_pieces)


def ladder_kernel(place_ref, b_ref, *rest):
    x_refs, (own_ref, oth_ref, g_ref, acc_ref, now_ref) = rest[:X_REFS], rest[X_REFS:]
    step = pl.program_id(0)

    @pl.when(step == 0)
    def _():
        for xx in range(NX):
            for half in range(2):
                tiles = [
                    b_ref[xx * NY + yy, :, pl.ds(half * LANE, LANE)].astype(F32)
                    for yy in range(NY)
                ]
                for g in range(4):
                    g_ref[half * 4 + g, :, pl.ds(xx * LANE, LANE)] = regroup(tiles, g).astype(BF)
        acc_ref[...] = jnp.zeros_like(acc_ref)

    def body(x):
        acc_ref[...] += lax.dot_general(
            g_ref[level_of(step, place_ref)],
            x,
            (((1,), (1,)), ((), ())),
            preferred_element_type=F32,
        )

    with_block(step, place_ref, x_refs, now_ref, body)

    @pl.when(step == NZ - 1)
    def _():
        core = place_ref[0]
        own_ref[...] = acc_ref[pl.ds(pl.multiple_of(core * HALF, HALF), HALF), :]
        oth_ref[...] = acc_ref[pl.ds(pl.multiple_of((1 - core) * HALF, HALF), HALF), :]


def make_ladder(place, b_all, xs):
    flat = pl.BlockSpec((HALF, WIDE), lambda k, p: (0, 0))
    return pl.pallas_call(
        ladder_kernel,
        out_shape=(
            jax.ShapeDtypeStruct((HALF, WIDE), F32),
            jax.ShapeDtypeStruct((HALF, WIDE), F32),
        ),
        grid_spec=pltpu.PrefetchScalarGridSpec(
            num_scalar_prefetch=1,
            grid=(NZ,),
            in_specs=[pl.BlockSpec((NV, PAD, HALF_M), lambda k, p: (0, 0, 0))] + x_specs(),
            out_specs=(flat, flat),
            scratch_shapes=[
                pltpu.VMEM((NZ, PAD, BLK), BF),
                pltpu.VMEM((PAD, WIDE), F32),
                NOW,
            ],
        ),
        compiler_params=pltpu.CompilerParams(dimension_semantics=("arbitrary",)),
        name="ladder",
    )(place, b_all, *xs)


def chunk_kernel(place_ref, own_ref, oth_ref, other_ref, col_ref, low_ref, out_ref):
    wide = own_ref[...] + oth_ref[...]
    lane = lax.broadcasted_iota(jnp.int32, (HALF, WIDE), 1)
    row = lax.broadcasted_iota(jnp.int32, (HALF, WIDE), 0)
    total = wide
    for v in range(1, NV):
        moved = pltpu.roll(wide, WIDE - v * (PAD - ROW), 1)
        total = jnp.where(lane >= v * ROW, moved, total)
    res = total[:, :NVIR] + other_ref[...]
    upd = res / (low_ref[...] + col_ref[...])
    real = row[:, :NVIR] + place_ref[0] * HALF < ROW
    upd = jnp.where(real, upd, 0.0)
    squares = jnp.sum(upd * upd, axis=1, keepdims=True)
    squares = jnp.sum(squares, axis=0, keepdims=True)
    high = squares.astype(BF).astype(F32)
    rest = squares - high
    mid = rest.astype(BF).astype(F32)
    low = rest - mid
    kept = jnp.where(lane == NVIR, high, jnp.where(lane == NVIR + 1, mid, low))
    kept = jnp.where((row == 0) & (lane < NVIR + 3), kept, 0.0)
    out_ref[...] = jnp.where(lane < NVIR, total, kept).astype(BF)


def make_chunk(place, own, oth, other_part, col_energy, low_energy):
    return pl.pallas_call(
        chunk_kernel,
        out_shape=jax.ShapeDtypeStruct((HALF, WIDE), BF),
        in_specs=[pl.BlockSpec(memory_space=pltpu.SMEM)]
        + [pl.BlockSpec(memory_space=pltpu.VMEM)] * 5,
        name="chunk",
    )(place, own, oth, other_part, col_energy, low_energy)


def final_kernel(place_ref, own_ref, oth_ref, other_ref, out_ref, mix_ref):
    def fill(source, start, count):
        for t in range(WIDE // LANE):
            lanes = min(LANE, NVIR - t * LANE)
            for i in range(PAIRS):
                mix_ref[t, pl.ds(i, HALF, stride=PAIRS), :] = source[
                    i, :, pl.ds(t * LANE, LANE)
                ].astype(F32)
            part = mix_ref[t, : count * PAIRS, :lanes].reshape(count, PAIRS, lanes)
            at = (pl.ds(start, count), slice(None), pl.ds(t * LANE, lanes))
            out_ref[at] = other_ref[at] + part

    @pl.when(place_ref[0] == 0)
    def _():
        fill(own_ref, 0, HALF)
        fill(oth_ref, HALF, ROW - HALF)

    @pl.when(place_ref[0] == 1)
    def _():
        fill(oth_ref, 0, HALF)
        fill(own_ref, HALF, ROW - HALF)


def make_final(place, l_own, l_oth, other_rows):
    return pl.pallas_call(
        final_kernel,
        out_shape=jax.ShapeDtypeStruct((ROW, PAIRS, NVIR), F32),
        in_specs=[pl.BlockSpec(memory_space=pltpu.SMEM)]
        + [pl.BlockSpec(memory_space=pltpu.VMEM)] * 3,
        scratch_shapes=[pltpu.VMEM((WIDE // LANE, HALF * PAIRS, LANE), F32)],
        name="residual",
    )(place, l_own, l_oth, other_rows)


def shards(amplitudes, factors, kernel, other_terms, virt_energy, pair_energy):
    core = lax.axis_index("c").astype(jnp.int32)
    level = lax.axis_index("z").astype(jnp.int32)
    place = jnp.stack(
        [core, level, lax.axis_index("x").astype(jnp.int32), lax.axis_index("y").astype(jnp.int32)]
    )

    x_pad = jnp.pad(factors, ((0, PAD - ROW), (0, 0)))
    z_cols = kernel.T.reshape(NV, QC, BLK)
    xz = jnp.concatenate([jnp.broadcast_to(x_pad[None], (NV, PAD, BLK)), z_cols], axis=1)
    x_pad, xz = lax.optimization_barrier((x_pad, xz))
    xz = lax.all_to_all(xz, XY, split_axis=0, concat_axis=0, tiled=True)
    t_pad = jnp.pad(amplitudes, ((0, 0), (0, PAD - ROW), (0, LANE - ROW)))[::-1]
    t_want = lax.dynamic_slice_in_dim(jnp.concatenate([t_pad, t_pad]), NZ - 1 - level, NZ, 0)
    far = {
        j: lax.ppermute(jnp.concatenate([x_pad, t_want[j]], axis=1), "z", ring(-j))
        for j in A_FAR + B_FAR
    }
    t_own = jnp.stack(
        [
            far[j][:, BLK:]
            if j in far
            else lax.ppermute(t_want[j], "z", ring(-j)) if j else t_want[0]
            for j in range(NZ)
        ]
    )
    t_oth = core_swap(t_own)
    a_parts = around(jnp.stack([far[j][:, :BLK] for j in A_FAR]), "x", "y")
    b_parts = around(jnp.stack([far[j][:, :BLK] for j in B_FAR]), "y", "x")
    x_own = xz[:, :PAD]
    x_up = lax.ppermute(x_own, "z", ring(-1))
    x_down = lax.ppermute(x_own, "z", ring(1))
    xs = (xz, x_up, x_down, *a_parts, *b_parts)

    z_all = xz.reshape(NZ, NC, PAD + QC, BLK)
    z_own = lax.dynamic_index_in_dim(z_all, core, 1, keepdims=False)[:, PAD:]
    z_oth = lax.dynamic_index_in_dim(z_all, 1 - core, 1, keepdims=False)[:, PAD:]
    z_here = jnp.stack([z_own, core_swap(z_oth)])
    ups, downs = [z_here], [z_here]
    for _ in range(3):
        ups.append(lax.ppermute(ups[-1], "z", ring(-1)))
        downs.append(lax.ppermute(downs[-1], "z", ring(1)))
    last_up = lax.ppermute(ups[-1][:1], "z", ring(-1))
    last_down = lax.ppermute(downs[-1][1:], "z", ring(1))
    z_pieces = (*ups, *downs[1:], last_up, last_down)

    h_msg = make_half(place, t_own, t_oth, xs)
    h_own = lax.all_to_all(h_msg, XY, split_axis=0, concat_axis=0, tiled=True)
    h_own = h_own.reshape(NV * PAD, HALF_M)
    h_oth = core_swap(h_own)

    b_own, b_send = make_main(place, h_own, h_oth, xs, z_pieces)
    b_sum = (b_own + core_swap(b_send).astype(F32)).astype(BF)
    b_all = lax.all_to_all(
        b_sum.reshape(NV, PAD, HALF_M), XY, split_axis=0, concat_axis=0, tiled=True
    )

    l_own, l_send = make_ladder(place, b_all, xs)
    l_recv = core_swap(l_send)
    other_part = lax.dynamic_index_in_dim(other_terms, level, 0, keepdims=False)
    other_part = jnp.pad(other_part, ((0, PAD - ROW), (0, 0)))
    other_part = lax.dynamic_slice_in_dim(other_part, core * HALF, HALF, 0)
    row_energy = lax.dynamic_slice_in_dim(virt_energy, lax.axis_index(XY) * ROW, ROW, 0)
    low_energy = jnp.pad(row_energy, (0, PAD - ROW), constant_values=1.0)
    low_energy = lax.dynamic_slice_in_dim(low_energy, core * HALF, HALF, 0)
    low_energy = (low_energy - lax.dynamic_index_in_dim(pair_energy, level, 0))[:, None]
    chunk = make_chunk(place, l_own, l_recv, other_part, virt_energy[None, :], low_energy)
    l_mine = lax.all_gather(chunk, "z", axis=0)
    l_rest = core_swap(l_mine)

    marks = jnp.concatenate([l_mine, l_rest])
    squares = jnp.sum(marks[:, 0, NVIR : NVIR + 3].astype(F32))
    total = jnp.broadcast_to(squares, (NV, 8, LANE))
    totals = lax.all_to_all(total, XY, split_axis=0, concat_axis=0, tiled=True)
    other_rows = jnp.transpose(other_terms, (1, 0, 2))
    residual = jnp.transpose(make_final(place, l_mine, l_rest, other_rows), (1, 0, 2))
    count = PAIRS * NVIR * NVIR
    update_rms = jnp.sqrt(jnp.sum(totals[:, 0, 0]) / count + epsilon)
    return residual, update_rms


def solution(mesh):
    torus = Mesh(mesh.devices.reshape(NX, NY, NZ, NC), AXES)
    return jax.shard_map(
        shards,
        mesh=torus,
        in_specs=(
            P(None, XY, RANK),
            P(XY, RANK),
            P(XY, RANK),
            P(None, XY, None),
            P(),
            P(),
        ),
        out_specs=(P(None, XY, None), P()),
        check_vma=False,
    )
```

```python
import jax
import jax.numpy as jnp
from jax import lax
from jax.experimental import pallas as pl
from jax.experimental.pallas import tpu as pltpu
from jax.sharding import Mesh
from jax.sharding import PartitionSpec as P

AXES = ("x", "y", "z", "c")
XY = ("x", "y")
RANK = ("z", "c")
BF = jnp.bfloat16
F32 = jnp.float32
epsilon = 1e-06


NX, NY, NZ, NC = 4, 4, 8, 2
NV = NX * NY
PAIRS = 8
ROW = 75
PAD = 80
BLK = 512
QC = 32
NVIR = 1200
LANE = 128
HALF = PAD // 2
WIDE = 1280


def core_swap(value):
    return lax.ppermute(value, "c", [(0, 1), (1, 0)])


def ring(shift):
    return [(s, (s + shift) % NZ) for s in range(NZ)]


def around(value, first, second):
    def step(piece, axis, shift):
        return lax.ppermute(piece, axis, [(s, (s + shift) % 4) for s in range(4)])

    left, right = step(value, first, 1), step(value, first, -1)
    cut = BLK // 2
    across = jnp.concatenate(
        [step(left[..., :cut], first, 1), step(right[..., cut:], first, -1)], axis=-1
    )
    line = jnp.stack([value, left, right, across])
    left, right = step(line, second, 1), step(line, second, -1)
    return line, left, right, step(left[:2], second, 1), step(right[2:], second, -1)


def regroup(tiles, want):
    out = None
    lane = lax.broadcasted_iota(jnp.int32, (PAD, LANE), 1) // QC
    for group, tile in enumerate(tiles):
        shift = ((group - want) * QC) % LANE
        moved = pltpu.roll(tile, shift, 1) if shift else tile
        out = moved if out is None else jnp.where(lane == group, moved, out)
    return out


NEAR = 3
A_FAR = (2, 3, 4)
B_FAR = (5, 6)
SHIFTS = (0, -1, 1, 2)
HALF_M = PAIRS * QC


def level_of(step, place):
    far = jnp.where(step == 2, NZ - 1, jnp.where(step > 2, step - 1, step))
    return (place[1] + far) % NZ


X_REFS = 13
X_SPECS = [pl.BlockSpec(memory_space=pl.ANY)] * X_REFS
SLOTS = [pltpu.VMEM((2, NV, PAD, BLK), BF), pltpu.SemaphoreType.DMA((2,))]


def x_block(step, place, x_refs, now_ref, sems):
    def send(source, target, slot):
        pltpu.make_async_copy(source, target, sems.at[slot]).start()

    def rows(refs, swapped, index, slot):
        parts = ((refs[0], 0, 0), (refs[1], -1, 0), (refs[2], 1, 0), (refs[3], 2, 0), (refs[4], 2, 2))
        for ref, outer, first in parts:
            for n in range(ref.shape[0]):
                inner = SHIFTS[first + n]
                dx, dy = (outer, inner) if swapped else (inner, outer)
                xx = (place[2] + (dx + NX)) % NX
                yy = (place[3] + (dy + NY)) % NY
                send(ref.at[n, index], now_ref.at[slot, xx * NY + yy], slot)

    def fetch(s, slot):
        @pl.when(s == 0)
        def _():
            send(x_refs[0].at[:, pl.ds(0, PAD), :], now_ref.at[slot], slot)

        @pl.when(s == 1)
        def _():
            send(x_refs[1], now_ref.at[slot], slot)

        @pl.when(s == 2)
        def _():
            send(x_refs[2], now_ref.at[slot], slot)

        @pl.when((s >= NEAR) & (s < NEAR + len(A_FAR)))
        def _():
            rows(x_refs[3:8], False, s - NEAR, slot)

        @pl.when((s >= NEAR + len(A_FAR)) & (s < NZ))
        def _():
            rows(x_refs[8:13], True, s - NEAR - len(A_FAR), slot)

    @pl.when(step == 0)
    def _():
        fetch(step, 0)

    fetch(step + 1, (step + 1) % 2)
    slot = step % 2
    pltpu.make_async_copy(now_ref.at[slot], now_ref.at[slot], sems.at[slot]).wait()
    return now_ref[slot].reshape(NV * PAD, BLK)


def half_kernel(place_ref, to_ref, tx_ref, *rest):
    x_refs, (out_ref, t_ref, tt_ref, acc_ref, now_ref, sems) = rest[:X_REFS], rest[X_REFS:]
    step = pl.program_id(0)
    core, level = place_ref[0], place_ref[1]

    @pl.when(step == 0)
    def _():
        for j in range(NZ):
            rank = 2 * ((level + j) % NZ)
            own = pl.multiple_of((rank + core) * PAD, PAD)
            oth = pl.multiple_of((rank + 1 - core) * PAD, PAD)
            t_ref[pl.ds(own, PAD), :] = to_ref[j].astype(F32).T[:PAD]
            t_ref[pl.ds(oth, PAD), :] = tx_ref[j].astype(F32).T[:PAD]
        tt_ref[...] = t_ref[...].T.astype(BF)

    def body(x):
        acc_ref[level_of(step, place_ref)] = jnp.dot(
            tt_ref[...], x, preferred_element_type=F32
        )

    body(x_block(step, place_ref, x_refs, now_ref, sems))

    @pl.when(step == NZ - 1)
    def _():
        for xx in range(NX):
            for half in range(2):
                tiles = [acc_ref[half * 4 + g, :, pl.ds(xx * LANE, LANE)] for g in range(4)]
                for yy in range(NY):
                    out_ref[xx * NY + yy, :, pl.ds(half * LANE, LANE)] = regroup(
                        tiles, yy
                    ).astype(BF)


def make_half(place, t_own, t_oth, xs):
    piece = pl.BlockSpec((NZ, PAD, LANE), lambda k, p: (0, 0, 0))
    return pl.pallas_call(
        half_kernel,
        out_shape=jax.ShapeDtypeStruct((NV, PAD, HALF_M), BF),
        grid_spec=pltpu.PrefetchScalarGridSpec(
            num_scalar_prefetch=1,
            grid=(NZ,),
            in_specs=[piece, piece] + X_SPECS,
            out_specs=pl.BlockSpec((NV, PAD, HALF_M), lambda k, p: (0, 0, 0)),
            scratch_shapes=[
                pltpu.VMEM((NV * PAD, PAD), F32),
                pltpu.VMEM((PAD, NV * PAD), BF),
                pltpu.VMEM((NZ, PAD, BLK), F32),
                *SLOTS,
            ],
        ),
        compiler_params=pltpu.CompilerParams(dimension_semantics=("arbitrary",)),
        name="half",
    )(place, t_own, t_oth, *xs)


def main_kernel(place_ref, ho_ref, hx_ref, *rest):
    x_refs, rest = rest[:X_REFS], rest[X_REFS:]
    pieces, (bo_ref, bx_ref, h_ref, z_ref, acc_ref, now_ref, sems) = rest[:-7], rest[-7:]
    step = pl.program_id(0)
    level = place_ref[1]

    @pl.when(step == 0)
    def _():
        h_ref[pl.ds(0, HALF_M), :] = ho_ref[...].astype(F32).T.astype(BF)
        h_ref[pl.ds(HALF_M, HALF_M), :] = hx_ref[...].astype(F32).T.astype(BF)
        acc_ref[...] = jnp.zeros_like(acc_ref)

    for (far, first, count), ref in zip(Z_PARTS, pieces):
        start = ((level + far) % NZ) * QC
        for j in range(count):
            at = pl.multiple_of((first + j) * HALF_M + start, QC)
            z_ref[pl.ds(at, QC), :] = ref[j, 0].astype(F32)

    def body(x):
        coupled = jnp.dot(h_ref[...], x, preferred_element_type=F32)
        w = (coupled * z_ref[...]).astype(BF)
        acc_ref[...] += lax.dot_general(
            x, w, (((1,), (1,)), ((), ())), preferred_element_type=F32
        )

    body(x_block(step, place_ref, x_refs, now_ref, sems))

    @pl.when(step == NZ - 1)
    def _():
        bo_ref[...] = acc_ref[:, :HALF_M]
        bx_ref[...] = acc_ref[:, HALF_M:].astype(BF)


Z_PARTS = (
    (0, 0, 2),
    (1, 0, 2),
    (2, 0, 2),
    (3, 0, 2),
    (7, 0, 2),
    (6, 0, 2),
    (5, 0, 2),
    (4, 0, 1),
    (4, 1, 1),
)


def make_main(place, h_own, h_oth, xs, z_pieces):
    rows = NV * PAD

    def z_spec(count):
        return pl.BlockSpec((count, 1, QC, BLK), lambda k, p: (0, level_of(k, p), 0, 0))

    flat = pl.BlockSpec((rows, HALF_M), lambda k, p: (0, 0))
    return pl.pallas_call(
        main_kernel,
        out_shape=(
            jax.ShapeDtypeStruct((rows, HALF_M), F32),
            jax.ShapeDtypeStruct((rows, HALF_M), BF),
        ),
        grid_spec=pltpu.PrefetchScalarGridSpec(
            num_scalar_prefetch=1,
            grid=(NZ,),
            in_specs=[flat, flat] + X_SPECS + [z_spec(part[2]) for part in Z_PARTS],
            out_specs=(flat, flat),
            scratch_shapes=[
                pltpu.VMEM((2 * HALF_M, rows), BF),
                pltpu.VMEM((2 * HALF_M, BLK), F32),
                pltpu.VMEM((rows, 2 * HALF_M), F32),
                *SLOTS,
            ],
        ),
        compiler_params=pltpu.CompilerParams(dimension_semantics=("arbitrary",)),
        cost_estimate=pl.CostEstimate(
            flops=4 * 512 * 1280 * 4096, bytes_accessed=18_000_000, transcendentals=0
        ),
        name="core",
    )(place, h_own, h_oth, *xs, *z_pieces)


def ladder_kernel(place_ref, b_ref, *rest):
    x_refs, (own_ref, oth_ref, g_ref, acc_ref, now_ref, sems) = rest[:X_REFS], rest[X_REFS:]
    step = pl.program_id(0)

    @pl.when(step == 0)
    def _():
        for xx in range(NX):
            for half in range(2):
                tiles = [
                    b_ref[xx * NY + yy, :, pl.ds(half * LANE, LANE)].astype(F32)
                    for yy in range(NY)
                ]
                for g in range(4):
                    g_ref[half * 4 + g, :, pl.ds(xx * LANE, LANE)] = regroup(tiles, g).astype(BF)
        acc_ref[...] = jnp.zeros_like(acc_ref)

    def body(x):
        acc_ref[...] += lax.dot_general(
            g_ref[level_of(step, place_ref)],
            x,
            (((1,), (1,)), ((), ())),
            preferred_element_type=F32,
        )

    body(x_block(step, place_ref, x_refs, now_ref, sems))

    @pl.when(step == NZ - 1)
    def _():
        core = place_ref[0]
        own_ref[...] = acc_ref[pl.ds(pl.multiple_of(core * HALF, HALF), HALF), :]
        oth_ref[...] = acc_ref[pl.ds(pl.multiple_of((1 - core) * HALF, HALF), HALF), :]


def make_ladder(place, b_all, xs):
    flat = pl.BlockSpec((HALF, WIDE), lambda k, p: (0, 0))
    return pl.pallas_call(
        ladder_kernel,
        out_shape=(
            jax.ShapeDtypeStruct((HALF, WIDE), F32),
            jax.ShapeDtypeStruct((HALF, WIDE), F32),
        ),
        grid_spec=pltpu.PrefetchScalarGridSpec(
            num_scalar_prefetch=1,
            grid=(NZ,),
            in_specs=[pl.BlockSpec((NV, PAD, HALF_M), lambda k, p: (0, 0, 0))] + X_SPECS,
            out_specs=(flat, flat),
            scratch_shapes=[
                pltpu.VMEM((NZ, PAD, BLK), BF),
                pltpu.VMEM((PAD, WIDE), F32),
                *SLOTS,
            ],
        ),
        compiler_params=pltpu.CompilerParams(dimension_semantics=("arbitrary",)),
        name="ladder",
    )(place, b_all, *xs)


def chunk_kernel(place_ref, own_ref, oth_ref, other_ref, col_ref, low_ref, out_ref):
    wide = own_ref[...] + oth_ref[...]
    lane = lax.broadcasted_iota(jnp.int32, (HALF, WIDE), 1)
    row = lax.broadcasted_iota(jnp.int32, (HALF, WIDE), 0)
    total = wide
    for v in range(1, NV):
        moved = pltpu.roll(wide, WIDE - v * (PAD - ROW), 1)
        total = jnp.where(lane >= v * ROW, moved, total)
    res = total[:, :NVIR] + other_ref[...]
    upd = res / (low_ref[...] + col_ref[...])
    real = row[:, :NVIR] + place_ref[0] * HALF < ROW
    upd = jnp.where(real, upd, 0.0)
    squares = jnp.sum(upd * upd, axis=1, keepdims=True)
    squares = jnp.sum(squares, axis=0, keepdims=True)
    high = squares.astype(BF).astype(F32)
    rest = squares - high
    mid = rest.astype(BF).astype(F32)
    low = rest - mid
    kept = jnp.where(lane == NVIR, high, jnp.where(lane == NVIR + 1, mid, low))
    kept = jnp.where((row == 0) & (lane < NVIR + 3), kept, 0.0)
    out_ref[...] = jnp.where(lane < NVIR, total, kept).astype(BF)


def make_chunk(place, own, oth, other_part, col_energy, low_energy):
    return pl.pallas_call(
        chunk_kernel,
        out_shape=jax.ShapeDtypeStruct((HALF, WIDE), BF),
        in_specs=[pl.BlockSpec(memory_space=pltpu.SMEM)]
        + [pl.BlockSpec(memory_space=pltpu.VMEM)] * 5,
        name="chunk",
    )(place, own, oth, other_part, col_energy, low_energy)


def final_kernel(place_ref, own_ref, oth_ref, other_ref, out_ref, mix_ref):
    def fill(source, start, count):
        for t in range(WIDE // LANE):
            lanes = min(LANE, NVIR - t * LANE)
            for i in range(PAIRS):
                mix_ref[t, pl.ds(i, HALF, stride=PAIRS), :] = source[
                    i, :, pl.ds(t * LANE, LANE)
                ].astype(F32)
            part = mix_ref[t, : count * PAIRS, :lanes].reshape(count, PAIRS, lanes)
            at = (pl.ds(start, count), slice(None), pl.ds(t * LANE, lanes))
            out_ref[at] = other_ref[at] + part

    @pl.when(place_ref[0] == 0)
    def _():
        fill(own_ref, 0, HALF)
        fill(oth_ref, HALF, ROW - HALF)

    @pl.when(place_ref[0] == 1)
    def _():
        fill(oth_ref, 0, HALF)
        fill(own_ref, HALF, ROW - HALF)


def make_final(place, l_own, l_oth, other_rows):
    return pl.pallas_call(
        final_kernel,
        out_shape=jax.ShapeDtypeStruct((ROW, PAIRS, NVIR), F32),
        in_specs=[pl.BlockSpec(memory_space=pltpu.SMEM)]
        + [pl.BlockSpec(memory_space=pltpu.VMEM)] * 3,
        scratch_shapes=[pltpu.VMEM((WIDE // LANE, HALF * PAIRS, LANE), F32)],
        name="residual",
    )(place, l_own, l_oth, other_rows)


def shards(amplitudes, factors, kernel, other_terms, virt_energy, pair_energy):
    core = lax.axis_index("c").astype(jnp.int32)
    level = lax.axis_index("z").astype(jnp.int32)
    place = jnp.stack(
        [core, level, lax.axis_index("x").astype(jnp.int32), lax.axis_index("y").astype(jnp.int32)]
    )

    x_pad = jnp.pad(factors, ((0, PAD - ROW), (0, 0)))
    z_cols = kernel.T.reshape(NV, QC, BLK)
    xz = jnp.concatenate([jnp.broadcast_to(x_pad[None], (NV, PAD, BLK)), z_cols], axis=1)
    x_pad, xz = lax.optimization_barrier((x_pad, xz))
    xz = lax.all_to_all(xz, XY, split_axis=0, concat_axis=0, tiled=True)
    t_pad = jnp.pad(amplitudes, ((0, 0), (0, PAD - ROW), (0, LANE - ROW)))[::-1]
    t_want = lax.dynamic_slice_in_dim(jnp.concatenate([t_pad, t_pad]), NZ - 1 - level, NZ, 0)
    far = {
        j: lax.ppermute(jnp.concatenate([x_pad, t_want[j]], axis=1), "z", ring(-j))
        for j in A_FAR + B_FAR
    }
    t_own = jnp.stack(
        [
            far[j][:, BLK:]
            if j in far
            else lax.ppermute(t_want[j], "z", ring(-j)) if j else t_want[0]
            for j in range(NZ)
        ]
    )
    t_oth = core_swap(t_own)
    a_parts = around(jnp.stack([far[j][:, :BLK] for j in A_FAR]), "x", "y")
    b_parts = around(jnp.stack([far[j][:, :BLK] for j in B_FAR]), "y", "x")
    x_own = xz[:, :PAD]
    x_up = lax.ppermute(x_own, "z", ring(-1))
    x_down = lax.ppermute(x_own, "z", ring(1))
    xs = (xz, x_up, x_down, *a_parts, *b_parts)

    z_all = xz.reshape(NZ, NC, PAD + QC, BLK)
    z_own = lax.dynamic_index_in_dim(z_all, core, 1, keepdims=False)[:, PAD:]
    z_oth = lax.dynamic_index_in_dim(z_all, 1 - core, 1, keepdims=False)[:, PAD:]
    z_here = jnp.stack([z_own, core_swap(z_oth)])
    ups, downs = [z_here], [z_here]
    for _ in range(3):
        ups.append(lax.ppermute(ups[-1], "z", ring(-1)))
        downs.append(lax.ppermute(downs[-1], "z", ring(1)))
    last_up = lax.ppermute(ups[-1][:1], "z", ring(-1))
    last_down = lax.ppermute(downs[-1][1:], "z", ring(1))
    z_pieces = (*ups, *downs[1:], last_up, last_down)

    h_msg = make_half(place, t_own, t_oth, xs)
    h_own = lax.all_to_all(h_msg, XY, split_axis=0, concat_axis=0, tiled=True)
    h_own = h_own.reshape(NV * PAD, HALF_M)
    h_oth = core_swap(h_own)

    b_own, b_send = make_main(place, h_own, h_oth, xs, z_pieces)
    b_sum = (b_own + core_swap(b_send).astype(F32)).astype(BF)
    b_all = lax.all_to_all(
        b_sum.reshape(NV, PAD, HALF_M), XY, split_axis=0, concat_axis=0, tiled=True
    )

    l_own, l_send = make_ladder(place, b_all, xs)
    l_recv = core_swap(l_send)
    other_part = lax.dynamic_index_in_dim(other_terms, level, 0, keepdims=False)
    other_part = jnp.pad(other_part, ((0, PAD - ROW), (0, 0)))
    other_part = lax.dynamic_slice_in_dim(other_part, core * HALF, HALF, 0)
    row_energy = lax.dynamic_slice_in_dim(virt_energy, lax.axis_index(XY) * ROW, ROW, 0)
    low_energy = jnp.pad(row_energy, (0, PAD - ROW), constant_values=1.0)
    low_energy = lax.dynamic_slice_in_dim(low_energy, core * HALF, HALF, 0)
    low_energy = (low_energy - lax.dynamic_index_in_dim(pair_energy, level, 0))[:, None]
    chunk = make_chunk(place, l_own, l_recv, other_part, virt_energy[None, :], low_energy)
    l_mine = lax.all_gather(chunk, "z", axis=0)
    l_rest = core_swap(l_mine)

    marks = jnp.concatenate([l_mine, l_rest])
    squares = jnp.sum(marks[:, 0, NVIR : NVIR + 3].astype(F32))
    total = jnp.broadcast_to(squares, (NV, 8, LANE))
    totals = lax.all_to_all(total, XY, split_axis=0, concat_axis=0, tiled=True)
    other_rows = jnp.transpose(other_terms, (1, 0, 2))
    residual = jnp.transpose(make_final(place, l_mine, l_rest, other_rows), (1, 0, 2))
    count = PAIRS * NVIR * NVIR
    update_rms = jnp.sqrt(jnp.sum(totals[:, 0, 0]) / count + epsilon)
    return residual, update_rms


def solution(mesh):
    torus = Mesh(mesh.devices.reshape(NX, NY, NZ, NC), AXES)
    return jax.shard_map(
        shards,
        mesh=torus,
        in_specs=(
            P(None, XY, RANK),
            P(XY, RANK),
            P(XY, RANK),
            P(None, XY, None),
            P(),
            P(),
        ),
        out_specs=(P(None, XY, None), P()),
        check_vma=False,
    )
```

```python
import jax
import jax.numpy as jnp
from jax import lax
from jax.experimental import pallas as pl
from jax.experimental.pallas import tpu as pltpu
from jax.sharding import Mesh
from jax.sharding import PartitionSpec as P

AXES = ("x", "y", "z", "c")
XY = ("x", "y")
RANK = ("z", "c")
BF = jnp.bfloat16
F32 = jnp.float32
epsilon = 1e-06


NX, NY, NZ, NC = 4, 4, 8, 2
NV = NX * NY
PAIRS = 8
ROW = 75
PAD = 80
BLK = 512
QC = 32
NVIR = 1200
LANE = 128
HALF = PAD // 2
WIDE = 1280


def core_swap(value):
    return lax.ppermute(value, "c", [(0, 1), (1, 0)])


def ring(shift):
    return [(s, (s + shift) % NZ) for s in range(NZ)]


def around(value, first, second):
    def step(piece, axis, shift):
        return lax.ppermute(piece, axis, [(s, (s + shift) % 4) for s in range(4)])

    left, right = step(value, first, 1), step(value, first, -1)
    cut = BLK // 2
    across = jnp.concatenate(
        [step(left[..., :cut], first, 1), step(right[..., cut:], first, -1)], axis=-1
    )
    line = jnp.stack([value, left, right, across])
    left, right = step(line, second, 1), step(line, second, -1)
    return line, left, right, step(left[:2], second, 1), step(right[2:], second, -1)


def regroup(tiles, want):
    out = None
    lane = lax.broadcasted_iota(jnp.int32, (PAD, LANE), 1) // QC
    for group, tile in enumerate(tiles):
        shift = ((group - want) * QC) % LANE
        moved = pltpu.roll(tile, shift, 1) if shift else tile
        out = moved if out is None else jnp.where(lane == group, moved, out)
    return out


NEAR = 3
A_FAR = (2, 3, 4)
B_FAR = (5, 6)
SHIFTS = (0, -1, 1, 2)
HALF_M = PAIRS * QC


def level_of(step, place):
    far = jnp.where(step == 2, NZ - 1, jnp.where(step > 2, step - 1, step))
    return (place[1] + far) % NZ


X_REFS = 13
X_SPECS = [pl.BlockSpec(memory_space=pl.ANY)] * X_REFS
SLOTS = [pltpu.VMEM((NZ, NV, PAD, BLK), BF), pltpu.SemaphoreType.DMA((NZ,))]


def x_block(step, place, x_refs, now_ref, sems):
    def send(source, target, slot):
        pltpu.make_async_copy(source, target, sems.at[slot]).start()

    def rows(refs, swapped, index, slot):
        parts = ((refs[0], 0, 0), (refs[1], -1, 0), (refs[2], 1, 0), (refs[3], 2, 0), (refs[4], 2, 2))
        for ref, outer, first in parts:
            for n in range(ref.shape[0]):
                inner = SHIFTS[first + n]
                dx, dy = (outer, inner) if swapped else (inner, outer)
                xx = (place[2] + (dx + NX)) % NX
                yy = (place[3] + (dy + NY)) % NY
                send(ref.at[n, index], now_ref.at[slot, xx * NY + yy], slot)

    @pl.when(step == 0)
    def _():
        send(x_refs[0].at[:, pl.ds(0, PAD), :], now_ref.at[0], 0)
        send(x_refs[1], now_ref.at[1], 1)
        send(x_refs[2], now_ref.at[2], 2)
        for n in range(len(A_FAR)):
            rows(x_refs[3:8], False, n, NEAR + n)
        for n in range(len(B_FAR)):
            rows(x_refs[8:13], True, n, NEAR + len(A_FAR) + n)

    pltpu.make_async_copy(now_ref.at[step], now_ref.at[step], sems.at[step]).wait()
    return now_ref[step].reshape(NV * PAD, BLK)


def half_kernel(place_ref, to_ref, tx_ref, *rest):
    x_refs, (out_ref, t_ref, tt_ref, acc_ref, now_ref, sems) = rest[:X_REFS], rest[X_REFS:]
    step = pl.program_id(0)
    core, level = place_ref[0], place_ref[1]

    @pl.when(step == 0)
    def _():
        for j in range(NZ):
            rank = 2 * ((level + j) % NZ)
            own = pl.multiple_of((rank + core) * PAD, PAD)
            oth = pl.multiple_of((rank + 1 - core) * PAD, PAD)
            t_ref[pl.ds(own, PAD), :] = to_ref[j].astype(F32).T[:PAD]
            t_ref[pl.ds(oth, PAD), :] = tx_ref[j].astype(F32).T[:PAD]
        tt_ref[...] = t_ref[...].T.astype(BF)

    def body(x):
        acc_ref[level_of(step, place_ref)] = jnp.dot(
            tt_ref[...], x, preferred_element_type=F32
        )

    body(x_block(step, place_ref, x_refs, now_ref, sems))

    @pl.when(step == NZ - 1)
    def _():
        for xx in range(NX):
            for half in range(2):
                tiles = [acc_ref[half * 4 + g, :, pl.ds(xx * LANE, LANE)] for g in range(4)]
                for yy in range(NY):
                    out_ref[xx * NY + yy, :, pl.ds(half * LANE, LANE)] = regroup(
                        tiles, yy
                    ).astype(BF)


def make_half(place, t_own, t_oth, xs):
    piece = pl.BlockSpec((NZ, PAD, LANE), lambda k, p: (0, 0, 0))
    return pl.pallas_call(
        half_kernel,
        out_shape=jax.ShapeDtypeStruct((NV, PAD, HALF_M), BF),
        grid_spec=pltpu.PrefetchScalarGridSpec(
            num_scalar_prefetch=1,
            grid=(NZ,),
            in_specs=[piece, piece] + X_SPECS,
            out_specs=pl.BlockSpec((NV, PAD, HALF_M), lambda k, p: (0, 0, 0)),
            scratch_shapes=[
                pltpu.VMEM((NV * PAD, PAD), F32),
                pltpu.VMEM((PAD, NV * PAD), BF),
                pltpu.VMEM((NZ, PAD, BLK), F32),
                *SLOTS,
            ],
        ),
        compiler_params=pltpu.CompilerParams(dimension_semantics=("arbitrary",)),
        name="half",
    )(place, t_own, t_oth, *xs)


def main_kernel(place_ref, ho_ref, hx_ref, *rest):
    x_refs, rest = rest[:X_REFS], rest[X_REFS:]
    pieces, (bo_ref, bx_ref, h_ref, z_ref, acc_ref, now_ref, sems) = rest[:-7], rest[-7:]
    step = pl.program_id(0)
    level = place_ref[1]

    @pl.when(step == 0)
    def _():
        h_ref[pl.ds(0, HALF_M), :] = ho_ref[...].astype(F32).T.astype(BF)
        h_ref[pl.ds(HALF_M, HALF_M), :] = hx_ref[...].astype(F32).T.astype(BF)
        acc_ref[...] = jnp.zeros_like(acc_ref)

    for (far, first, count), ref in zip(Z_PARTS, pieces):
        start = ((level + far) % NZ) * QC
        for j in range(count):
            at = pl.multiple_of((first + j) * HALF_M + start, QC)
            z_ref[pl.ds(at, QC), :] = ref[j, 0].astype(F32)

    def body(x):
        coupled = jnp.dot(h_ref[...], x, preferred_element_type=F32)
        w = (coupled * z_ref[...]).astype(BF)
        acc_ref[...] += lax.dot_general(
            x, w, (((1,), (1,)), ((), ())), preferred_element_type=F32
        )

    body(x_block(step, place_ref, x_refs, now_ref, sems))

    @pl.when(step == NZ - 1)
    def _():
        bo_ref[...] = acc_ref[:, :HALF_M]
        bx_ref[...] = acc_ref[:, HALF_M:].astype(BF)


Z_PARTS = (
    (0, 0, 2),
    (1, 0, 2),
    (2, 0, 2),
    (3, 0, 2),
    (7, 0, 2),
    (6, 0, 2),
    (5, 0, 2),
    (4, 0, 1),
    (4, 1, 1),
)


def make_main(place, h_own, h_oth, xs, z_pieces):
    rows = NV * PAD

    def z_spec(count):
        return pl.BlockSpec((count, 1, QC, BLK), lambda k, p: (0, level_of(k, p), 0, 0))

    flat = pl.BlockSpec((rows, HALF_M), lambda k, p: (0, 0))
    return pl.pallas_call(
        main_kernel,
        out_shape=(
            jax.ShapeDtypeStruct((rows, HALF_M), F32),
            jax.ShapeDtypeStruct((rows, HALF_M), BF),
        ),
        grid_spec=pltpu.PrefetchScalarGridSpec(
            num_scalar_prefetch=1,
            grid=(NZ,),
            in_specs=[flat, flat] + X_SPECS + [z_spec(part[2]) for part in Z_PARTS],
            out_specs=(flat, flat),
            scratch_shapes=[
                pltpu.VMEM((2 * HALF_M, rows), BF),
                pltpu.VMEM((2 * HALF_M, BLK), F32),
                pltpu.VMEM((rows, 2 * HALF_M), F32),
                *SLOTS,
            ],
        ),
        compiler_params=pltpu.CompilerParams(dimension_semantics=("arbitrary",)),
        cost_estimate=pl.CostEstimate(
            flops=4 * 512 * 1280 * 4096, bytes_accessed=18_000_000, transcendentals=0
        ),
        name="core",
    )(place, h_own, h_oth, *xs, *z_pieces)


def ladder_kernel(place_ref, b_ref, *rest):
    x_refs, (own_ref, oth_ref, g_ref, acc_ref, now_ref, sems) = rest[:X_REFS], rest[X_REFS:]
    step = pl.program_id(0)

    @pl.when(step == 0)
    def _():
        for xx in range(NX):
            for half in range(2):
                tiles = [
                    b_ref[xx * NY + yy, :, pl.ds(half * LANE, LANE)].astype(F32)
                    for yy in range(NY)
                ]
                for g in range(4):
                    g_ref[half * 4 + g, :, pl.ds(xx * LANE, LANE)] = regroup(tiles, g).astype(BF)
        acc_ref[...] = jnp.zeros_like(acc_ref)

    def body(x):
        acc_ref[...] += lax.dot_general(
            g_ref[level_of(step, place_ref)],
            x,
            (((1,), (1,)), ((), ())),
            preferred_element_type=F32,
        )

    body(x_block(step, place_ref, x_refs, now_ref, sems))

    @pl.when(step == NZ - 1)
    def _():
        core = place_ref[0]
        own_ref[...] = acc_ref[pl.ds(pl.multiple_of(core * HALF, HALF), HALF), :]
        oth_ref[...] = acc_ref[pl.ds(pl.multiple_of((1 - core) * HALF, HALF), HALF), :]


def make_ladder(place, b_all, xs):
    flat = pl.BlockSpec((HALF, WIDE), lambda k, p: (0, 0))
    return pl.pallas_call(
        ladder_kernel,
        out_shape=(
            jax.ShapeDtypeStruct((HALF, WIDE), F32),
            jax.ShapeDtypeStruct((HALF, WIDE), F32),
        ),
        grid_spec=pltpu.PrefetchScalarGridSpec(
            num_scalar_prefetch=1,
            grid=(NZ,),
            in_specs=[pl.BlockSpec((NV, PAD, HALF_M), lambda k, p: (0, 0, 0))] + X_SPECS,
            out_specs=(flat, flat),
            scratch_shapes=[
                pltpu.VMEM((NZ, PAD, BLK), BF),
                pltpu.VMEM((PAD, WIDE), F32),
                *SLOTS,
            ],
        ),
        compiler_params=pltpu.CompilerParams(dimension_semantics=("arbitrary",)),
        name="ladder",
    )(place, b_all, *xs)


def chunk_kernel(place_ref, own_ref, oth_ref, other_ref, col_ref, low_ref, out_ref):
    wide = own_ref[...] + oth_ref[...]
    lane = lax.broadcasted_iota(jnp.int32, (HALF, WIDE), 1)
    row = lax.broadcasted_iota(jnp.int32, (HALF, WIDE), 0)
    total = wide
    for v in range(1, NV):
        moved = pltpu.roll(wide, WIDE - v * (PAD - ROW), 1)
        total = jnp.where(lane >= v * ROW, moved, total)
    res = total[:, :NVIR] + other_ref[...]
    upd = res / (low_ref[...] + col_ref[...])
    real = row[:, :NVIR] + place_ref[0] * HALF < ROW
    upd = jnp.where(real, upd, 0.0)
    squares = jnp.sum(upd * upd, axis=1, keepdims=True)
    squares = jnp.sum(squares, axis=0, keepdims=True)
    high = squares.astype(BF).astype(F32)
    rest = squares - high
    mid = rest.astype(BF).astype(F32)
    low = rest - mid
    kept = jnp.where(lane == NVIR, high, jnp.where(lane == NVIR + 1, mid, low))
    kept = jnp.where((row == 0) & (lane < NVIR + 3), kept, 0.0)
    out_ref[...] = jnp.where(lane < NVIR, total, kept).astype(BF)


def make_chunk(place, own, oth, other_part, col_energy, low_energy):
    return pl.pallas_call(
        chunk_kernel,
        out_shape=jax.ShapeDtypeStruct((HALF, WIDE), BF),
        in_specs=[pl.BlockSpec(memory_space=pltpu.SMEM)]
        + [pl.BlockSpec(memory_space=pltpu.VMEM)] * 5,
        name="chunk",
    )(place, own, oth, other_part, col_energy, low_energy)


def final_kernel(place_ref, own_ref, oth_ref, other_ref, out_ref, mix_ref):
    def fill(source, start, count):
        for t in range(WIDE // LANE):
            lanes = min(LANE, NVIR - t * LANE)
            for i in range(PAIRS):
                mix_ref[t, pl.ds(i, HALF, stride=PAIRS), :] = source[
                    i, :, pl.ds(t * LANE, LANE)
                ].astype(F32)
            part = mix_ref[t, : count * PAIRS, :lanes].reshape(count, PAIRS, lanes)
            at = (pl.ds(start, count), slice(None), pl.ds(t * LANE, lanes))
            out_ref[at] = other_ref[at] + part

    @pl.when(place_ref[0] == 0)
    def _():
        fill(own_ref, 0, HALF)
        fill(oth_ref, HALF, ROW - HALF)

    @pl.when(place_ref[0] == 1)
    def _():
        fill(oth_ref, 0, HALF)
        fill(own_ref, HALF, ROW - HALF)


def make_final(place, l_own, l_oth, other_rows):
    return pl.pallas_call(
        final_kernel,
        out_shape=jax.ShapeDtypeStruct((ROW, PAIRS, NVIR), F32),
        in_specs=[pl.BlockSpec(memory_space=pltpu.SMEM)]
        + [pl.BlockSpec(memory_space=pltpu.VMEM)] * 3,
        scratch_shapes=[pltpu.VMEM((WIDE // LANE, HALF * PAIRS, LANE), F32)],
        name="residual",
    )(place, l_own, l_oth, other_rows)


def shards(amplitudes, factors, kernel, other_terms, virt_energy, pair_energy):
    core = lax.axis_index("c").astype(jnp.int32)
    level = lax.axis_index("z").astype(jnp.int32)
    place = jnp.stack(
        [core, level, lax.axis_index("x").astype(jnp.int32), lax.axis_index("y").astype(jnp.int32)]
    )

    x_pad = jnp.pad(factors, ((0, PAD - ROW), (0, 0)))
    z_cols = kernel.T.reshape(NV, QC, BLK)
    xz = jnp.concatenate([jnp.broadcast_to(x_pad[None], (NV, PAD, BLK)), z_cols], axis=1)
    x_pad, xz = lax.optimization_barrier((x_pad, xz))
    xz = lax.all_to_all(xz, XY, split_axis=0, concat_axis=0, tiled=True)
    t_pad = jnp.pad(amplitudes, ((0, 0), (0, PAD - ROW), (0, LANE - ROW)))[::-1]
    t_want = lax.dynamic_slice_in_dim(jnp.concatenate([t_pad, t_pad]), NZ - 1 - level, NZ, 0)
    far = {
        j: lax.ppermute(jnp.concatenate([x_pad, t_want[j]], axis=1), "z", ring(-j))
        for j in A_FAR + B_FAR
    }
    t_own = jnp.stack(
        [
            far[j][:, BLK:]
            if j in far
            else lax.ppermute(t_want[j], "z", ring(-j)) if j else t_want[0]
            for j in range(NZ)
        ]
    )
    t_oth = core_swap(t_own)
    a_parts = around(jnp.stack([far[j][:, :BLK] for j in A_FAR]), "x", "y")
    b_parts = around(jnp.stack([far[j][:, :BLK] for j in B_FAR]), "y", "x")
    x_own = xz[:, :PAD]
    x_up = lax.ppermute(x_own, "z", ring(-1))
    x_down = lax.ppermute(x_own, "z", ring(1))
    xs = (xz, x_up, x_down, *a_parts, *b_parts)

    z_all = xz.reshape(NZ, NC, PAD + QC, BLK)
    z_own = lax.dynamic_index_in_dim(z_all, core, 1, keepdims=False)[:, PAD:]
    z_oth = lax.dynamic_index_in_dim(z_all, 1 - core, 1, keepdims=False)[:, PAD:]
    z_here = jnp.stack([z_own, core_swap(z_oth)])
    ups, downs = [z_here], [z_here]
    for _ in range(3):
        ups.append(lax.ppermute(ups[-1], "z", ring(-1)))
        downs.append(lax.ppermute(downs[-1], "z", ring(1)))
    last_up = lax.ppermute(ups[-1][:1], "z", ring(-1))
    last_down = lax.ppermute(downs[-1][1:], "z", ring(1))
    z_pieces = (*ups, *downs[1:], last_up, last_down)

    h_msg = make_half(place, t_own, t_oth, xs)
    h_own = lax.all_to_all(h_msg, XY, split_axis=0, concat_axis=0, tiled=True)
    h_own = h_own.reshape(NV * PAD, HALF_M)
    h_oth = core_swap(h_own)

    b_own, b_send = make_main(place, h_own, h_oth, xs, z_pieces)
    b_sum = (b_own + core_swap(b_send).astype(F32)).astype(BF)
    b_all = lax.all_to_all(
        b_sum.reshape(NV, PAD, HALF_M), XY, split_axis=0, concat_axis=0, tiled=True
    )

    l_own, l_send = make_ladder(place, b_all, xs)
    l_recv = core_swap(l_send)
    other_part = lax.dynamic_index_in_dim(other_terms, level, 0, keepdims=False)
    other_part = jnp.pad(other_part, ((0, PAD - ROW), (0, 0)))
    other_part = lax.dynamic_slice_in_dim(other_part, core * HALF, HALF, 0)
    row_energy = lax.dynamic_slice_in_dim(virt_energy, lax.axis_index(XY) * ROW, ROW, 0)
    low_energy = jnp.pad(row_energy, (0, PAD - ROW), constant_values=1.0)
    low_energy = lax.dynamic_slice_in_dim(low_energy, core * HALF, HALF, 0)
    low_energy = (low_energy - lax.dynamic_index_in_dim(pair_energy, level, 0))[:, None]
    chunk = make_chunk(place, l_own, l_recv, other_part, virt_energy[None, :], low_energy)
    l_mine = lax.all_gather(chunk, "z", axis=0)
    l_rest = core_swap(l_mine)

    marks = jnp.concatenate([l_mine, l_rest])
    squares = jnp.sum(marks[:, 0, NVIR : NVIR + 3].astype(F32))
    total = jnp.broadcast_to(squares, (NV, 8, LANE))
    totals = lax.all_to_all(total, XY, split_axis=0, concat_axis=0, tiled=True)
    other_rows = jnp.transpose(other_terms, (1, 0, 2))
    residual = jnp.transpose(make_final(place, l_mine, l_rest, other_rows), (1, 0, 2))
    count = PAIRS * NVIR * NVIR
    update_rms = jnp.sqrt(jnp.sum(totals[:, 0, 0]) / count + epsilon)
    return residual, update_rms


def solution(mesh):
    torus = Mesh(mesh.devices.reshape(NX, NY, NZ, NC), AXES)
    return jax.shard_map(
        shards,
        mesh=torus,
        in_specs=(
            P(None, XY, RANK),
            P(XY, RANK),
            P(XY, RANK),
            P(None, XY, None),
            P(),
            P(),
        ),
        out_specs=(P(None, XY, None), P()),
        check_vma=False,
    )
```

```python
import jax
import jax.numpy as jnp
from jax import lax
from jax.experimental import pallas as pl
from jax.experimental.pallas import tpu as pltpu
from jax.sharding import Mesh
from jax.sharding import PartitionSpec as P

AXES = ("x", "y", "z", "c")
XY = ("x", "y")
RANK = ("z", "c")
BF = jnp.bfloat16
F32 = jnp.float32
epsilon = 1e-06


NX, NY, NZ, NC = 4, 4, 8, 2
NV = NX * NY
PAIRS = 8
ROW = 75
PAD = 80
BLK = 512
QC = 32
NVIR = 1200
LANE = 128
HALF = PAD // 2
WIDE = 1280


def core_swap(value):
    return lax.ppermute(value, "c", [(0, 1), (1, 0)])


def ring(shift):
    return [(s, (s + shift) % NZ) for s in range(NZ)]


def around(value, first, second):
    def step(piece, axis, shift):
        return lax.ppermute(piece, axis, [(s, (s + shift) % 4) for s in range(4)])

    left, right = step(value, first, 1), step(value, first, -1)
    cut = BLK // 2
    across = jnp.concatenate(
        [step(left[..., :cut], first, 1), step(right[..., cut:], first, -1)], axis=-1
    )
    line = jnp.stack([value, left, right, across])
    left, right = step(line, second, 1), step(line, second, -1)
    return line, left, right, step(left[:2], second, 1), step(right[2:], second, -1)


def regroup(tiles, want):
    out = None
    lane = lax.broadcasted_iota(jnp.int32, (PAD, LANE), 1) // QC
    for group, tile in enumerate(tiles):
        shift = ((group - want) * QC) % LANE
        moved = pltpu.roll(tile, shift, 1) if shift else tile
        out = moved if out is None else jnp.where(lane == group, moved, out)
    return out


NEAR = 3
A_FAR = (2, 3, 4)
B_FAR = (5, 6)
SHIFTS = (0, -1, 1, 2)
HALF_M = PAIRS * QC


def level_of(step, place):
    far = jnp.where(step == 2, NZ - 1, jnp.where(step > 2, step - 1, step))
    return (place[1] + far) % NZ


X_REFS = 13
X_SPECS = [pl.BlockSpec(memory_space=pl.ANY)] * X_REFS
SLOTS = [pltpu.VMEM((NZ, NV, PAD, BLK), BF), pltpu.SemaphoreType.DMA((NZ,))]


def fetch_all(place, x_refs, now_ref, sems):
    def send(source, target, slot):
        pltpu.make_async_copy(source, target, sems.at[slot]).start()

    def rows(refs, swapped, index, slot):
        parts = ((refs[0], 0, 0), (refs[1], -1, 0), (refs[2], 1, 0), (refs[3], 2, 0), (refs[4], 2, 2))
        for ref, outer, first in parts:
            for n in range(ref.shape[0]):
                inner = SHIFTS[first + n]
                dx, dy = (outer, inner) if swapped else (inner, outer)
                xx = (place[2] + (dx + NX)) % NX
                yy = (place[3] + (dy + NY)) % NY
                send(ref.at[n, index], now_ref.at[slot, xx * NY + yy], slot)

    send(x_refs[0].at[:, pl.ds(0, PAD), :], now_ref.at[0], 0)
    send(x_refs[1], now_ref.at[1], 1)
    send(x_refs[2], now_ref.at[2], 2)

    @pl.loop(0, len(A_FAR))
    def _(n):
        rows(x_refs[3:8], False, n, NEAR + n)

    @pl.loop(0, len(B_FAR))
    def _(n):
        rows(x_refs[8:13], True, n, NEAR + len(A_FAR) + n)


def fetched(step, now_ref, sems):
    pltpu.make_async_copy(now_ref.at[step], now_ref.at[step], sems.at[step]).wait()
    return now_ref[step].reshape(NV * PAD, BLK)


def half_kernel(place_ref, to_ref, tx_ref, *rest):
    x_refs, (out_ref, t_ref, tt_ref, acc_ref, now_ref, sems) = rest[:X_REFS], rest[X_REFS:]
    step = pl.program_id(0)
    core, level = place_ref[0], place_ref[1]

    @pl.when(step == 0)
    def _():
        fetch_all(place_ref, x_refs, now_ref, sems)
        for j in range(NZ):
            rank = 2 * ((level + j) % NZ)
            own = pl.multiple_of((rank + core) * PAD, PAD)
            oth = pl.multiple_of((rank + 1 - core) * PAD, PAD)
            t_ref[pl.ds(own, PAD), :] = to_ref[j].astype(F32).T[:PAD]
            t_ref[pl.ds(oth, PAD), :] = tx_ref[j].astype(F32).T[:PAD]
        tt_ref[...] = t_ref[...].T.astype(BF)

    def body(x):
        acc_ref[level_of(step, place_ref)] = jnp.dot(
            tt_ref[...], x, preferred_element_type=F32
        )

    body(fetched(step, now_ref, sems))

    @pl.when(step == NZ - 1)
    def _():
        for xx in range(NX):
            for half in range(2):
                tiles = [acc_ref[half * 4 + g, :, pl.ds(xx * LANE, LANE)] for g in range(4)]
                for yy in range(NY):
                    out_ref[xx * NY + yy, :, pl.ds(half * LANE, LANE)] = regroup(
                        tiles, yy
                    ).astype(BF)


def make_half(place, t_own, t_oth, xs):
    piece = pl.BlockSpec((NZ, PAD, LANE), lambda k, p: (0, 0, 0))
    return pl.pallas_call(
        half_kernel,
        out_shape=jax.ShapeDtypeStruct((NV, PAD, HALF_M), BF),
        grid_spec=pltpu.PrefetchScalarGridSpec(
            num_scalar_prefetch=1,
            grid=(NZ,),
            in_specs=[piece, piece] + X_SPECS,
            out_specs=pl.BlockSpec((NV, PAD, HALF_M), lambda k, p: (0, 0, 0)),
            scratch_shapes=[
                pltpu.VMEM((NV * PAD, PAD), F32),
                pltpu.VMEM((PAD, NV * PAD), BF),
                pltpu.VMEM((NZ, PAD, BLK), F32),
                *SLOTS,
            ],
        ),
        compiler_params=pltpu.CompilerParams(dimension_semantics=("arbitrary",)),
        name="half",
    )(place, t_own, t_oth, *xs)


def main_kernel(place_ref, ho_ref, hx_ref, *rest):
    x_refs, rest = rest[:X_REFS], rest[X_REFS:]
    pieces, rest = rest[: len(Z_PARTS)], rest[len(Z_PARTS) :]
    bo_ref, bx_ref, h_ref, acc_ref, z_ref, z_sem, now_ref, sems = rest
    step = pl.program_id(0)
    level = place_ref[1]

    @pl.when(step == 0)
    def _():
        for (far, first, count), ref in zip(Z_PARTS, pieces):
            for j in range(count):
                target = z_ref.at[:, first + j, (level + far) % NZ]
                pltpu.make_async_copy(ref.at[j], target, z_sem).start()
        fetch_all(place_ref, x_refs, now_ref, sems)
        h_ref[pl.ds(0, HALF_M), :] = ho_ref[...].astype(F32).T.astype(BF)
        h_ref[pl.ds(HALF_M, HALF_M), :] = hx_ref[...].astype(F32).T.astype(BF)
        acc_ref[...] = jnp.zeros_like(acc_ref)
        pltpu.make_async_copy(z_ref, z_ref, z_sem).wait()

    def weighted(k):
        x = fetched(k, now_ref, sems)
        coupled = jnp.dot(h_ref[...], x, preferred_element_type=F32)
        z = z_ref[level_of(k, place_ref)].reshape(2 * HALF_M, BLK).astype(F32)
        return x, (coupled * z).astype(BF)

    def back(x, w):
        return lax.dot_general(x, w, (((1,), (1,)), ((), ())), preferred_element_type=F32)

    x0, w0 = weighted(2 * step)
    x1, w1 = weighted(2 * step + 1)
    acc_ref[...] += back(x0, w0) + back(x1, w1)

    @pl.when(step == NZ // 2 - 1)
    def _():
        bo_ref[...] = acc_ref[:, :HALF_M]
        bx_ref[...] = acc_ref[:, HALF_M:].astype(BF)


Z_PARTS = (
    (0, 0, 2),
    (1, 0, 2),
    (2, 0, 2),
    (3, 0, 2),
    (7, 0, 2),
    (6, 0, 2),
    (5, 0, 2),
    (4, 0, 1),
    (4, 1, 1),
)


def make_main(place, h_own, h_oth, xs, z_pieces):
    rows = NV * PAD
    flat = pl.BlockSpec((rows, HALF_M), lambda k, p: (0, 0))
    return pl.pallas_call(
        main_kernel,
        out_shape=(
            jax.ShapeDtypeStruct((rows, HALF_M), F32),
            jax.ShapeDtypeStruct((rows, HALF_M), BF),
        ),
        grid_spec=pltpu.PrefetchScalarGridSpec(
            num_scalar_prefetch=1,
            grid=(NZ // 2,),
            in_specs=[flat, flat] + X_SPECS + [pl.BlockSpec(memory_space=pl.ANY)] * len(Z_PARTS),
            out_specs=(flat, flat),
            scratch_shapes=[
                pltpu.VMEM((2 * HALF_M, rows), BF),
                pltpu.VMEM((rows, 2 * HALF_M), F32),
                pltpu.VMEM((NZ, NC, NZ, QC, BLK), BF),
                pltpu.SemaphoreType.DMA,
                *SLOTS,
            ],
        ),
        compiler_params=pltpu.CompilerParams(dimension_semantics=("arbitrary",)),
        cost_estimate=pl.CostEstimate(
            flops=4 * 512 * 1280 * 4096, bytes_accessed=18_000_000, transcendentals=0
        ),
        name="core",
    )(place, h_own, h_oth, *xs, *z_pieces)


def ladder_kernel(place_ref, b_ref, *rest):
    x_refs, (own_ref, oth_ref, g_ref, acc_ref, now_ref, sems) = rest[:X_REFS], rest[X_REFS:]
    step = pl.program_id(0)

    @pl.when(step == 0)
    def _():
        fetch_all(place_ref, x_refs, now_ref, sems)
        for xx in range(NX):
            for half in range(2):
                tiles = [
                    b_ref[xx * NY + yy, :, pl.ds(half * LANE, LANE)].astype(F32)
                    for yy in range(NY)
                ]
                for g in range(4):
                    g_ref[half * 4 + g, :, pl.ds(xx * LANE, LANE)] = regroup(tiles, g).astype(BF)
        acc_ref[...] = jnp.zeros_like(acc_ref)

    def body(x):
        acc_ref[...] += lax.dot_general(
            g_ref[level_of(step, place_ref)],
            x,
            (((1,), (1,)), ((), ())),
            preferred_element_type=F32,
        )

    body(fetched(step, now_ref, sems))

    @pl.when(step == NZ - 1)
    def _():
        core = place_ref[0]
        own_ref[...] = acc_ref[pl.ds(pl.multiple_of(core * HALF, HALF), HALF), :]
        oth_ref[...] = acc_ref[pl.ds(pl.multiple_of((1 - core) * HALF, HALF), HALF), :]


def make_ladder(place, b_all, xs):
    flat = pl.BlockSpec((HALF, WIDE), lambda k, p: (0, 0))
    return pl.pallas_call(
        ladder_kernel,
        out_shape=(
            jax.ShapeDtypeStruct((HALF, WIDE), F32),
            jax.ShapeDtypeStruct((HALF, WIDE), F32),
        ),
        grid_spec=pltpu.PrefetchScalarGridSpec(
            num_scalar_prefetch=1,
            grid=(NZ,),
            in_specs=[pl.BlockSpec((NV, PAD, HALF_M), lambda k, p: (0, 0, 0))] + X_SPECS,
            out_specs=(flat, flat),
            scratch_shapes=[
                pltpu.VMEM((NZ, PAD, BLK), BF),
                pltpu.VMEM((PAD, WIDE), F32),
                *SLOTS,
            ],
        ),
        compiler_params=pltpu.CompilerParams(dimension_semantics=("arbitrary",)),
        name="ladder",
    )(place, b_all, *xs)


def chunk_kernel(place_ref, own_ref, oth_ref, other_ref, col_ref, low_ref, out_ref):
    wide = own_ref[...] + oth_ref[...]
    lane = lax.broadcasted_iota(jnp.int32, (HALF, WIDE), 1)
    row = lax.broadcasted_iota(jnp.int32, (HALF, WIDE), 0)
    total = wide
    for v in range(1, NV):
        moved = pltpu.roll(wide, WIDE - v * (PAD - ROW), 1)
        total = jnp.where(lane >= v * ROW, moved, total)
    res = total[:, :NVIR] + other_ref[...]
    upd = res / (low_ref[...] + col_ref[...])
    real = row[:, :NVIR] + place_ref[0] * HALF < ROW
    upd = jnp.where(real, upd, 0.0)
    squares = jnp.sum(upd * upd, axis=1, keepdims=True)
    squares = jnp.sum(squares, axis=0, keepdims=True)
    high = squares.astype(BF).astype(F32)
    rest = squares - high
    mid = rest.astype(BF).astype(F32)
    low = rest - mid
    kept = jnp.where(lane == NVIR, high, jnp.where(lane == NVIR + 1, mid, low))
    kept = jnp.where((row == 0) & (lane < NVIR + 3), kept, 0.0)
    out_ref[...] = jnp.where(lane < NVIR, total, kept).astype(BF)


def make_chunk(place, own, oth, other_part, col_energy, low_energy):
    return pl.pallas_call(
        chunk_kernel,
        out_shape=jax.ShapeDtypeStruct((HALF, WIDE), BF),
        in_specs=[pl.BlockSpec(memory_space=pltpu.SMEM)]
        + [pl.BlockSpec(memory_space=pltpu.VMEM)] * 5,
        name="chunk",
    )(place, own, oth, other_part, col_energy, low_energy)


def final_kernel(place_ref, own_ref, oth_ref, other_ref, out_ref, mix_ref):
    both = ROW - HALF

    def fill(source, start):
        for t in range(WIDE // LANE):
            lanes = min(LANE, NVIR - t * LANE)
            for i in range(PAIRS):
                mix_ref[t, pl.ds(i, HALF, stride=PAIRS), :] = source[
                    i, :, pl.ds(t * LANE, LANE)
                ].astype(F32)
            part = mix_ref[t, : both * PAIRS, :lanes].reshape(both, PAIRS, lanes)
            at = (pl.ds(start, both), slice(None), pl.ds(t * LANE, lanes))
            out_ref[at] = other_ref[at] + part

        @pl.when(start == 0)
        def _():
            for t in range(WIDE // LANE):
                lanes = min(LANE, NVIR - t * LANE)
                part = mix_ref[t, both * PAIRS :, :lanes].reshape(HALF - both, PAIRS, lanes)
                at = (pl.ds(both, HALF - both), slice(None), pl.ds(t * LANE, lanes))
                out_ref[at] = other_ref[at] + part

    fill(own_ref, place_ref[0] * HALF)
    fill(oth_ref, (1 - place_ref[0]) * HALF)


def make_final(place, l_own, l_oth, other_rows):
    return pl.pallas_call(
        final_kernel,
        out_shape=jax.ShapeDtypeStruct((ROW, PAIRS, NVIR), F32),
        in_specs=[pl.BlockSpec(memory_space=pltpu.SMEM)]
        + [pl.BlockSpec(memory_space=pltpu.VMEM)] * 3,
        scratch_shapes=[pltpu.VMEM((WIDE // LANE, HALF * PAIRS, LANE), F32)],
        name="residual",
    )(place, l_own, l_oth, other_rows)


def shards(amplitudes, factors, kernel, other_terms, virt_energy, pair_energy):
    core = lax.axis_index("c").astype(jnp.int32)
    level = lax.axis_index("z").astype(jnp.int32)
    place = jnp.stack(
        [core, level, lax.axis_index("x").astype(jnp.int32), lax.axis_index("y").astype(jnp.int32)]
    )

    x_pad = jnp.pad(factors, ((0, PAD - ROW), (0, 0)))
    z_cols = kernel.T.reshape(NV, QC, BLK)
    xz = jnp.concatenate([jnp.broadcast_to(x_pad[None], (NV, PAD, BLK)), z_cols], axis=1)
    x_pad, xz = lax.optimization_barrier((x_pad, xz))
    xz = lax.all_to_all(xz, XY, split_axis=0, concat_axis=0, tiled=True)
    t_pad = jnp.pad(amplitudes, ((0, 0), (0, PAD - ROW), (0, LANE - ROW)))[::-1]
    t_want = lax.dynamic_slice_in_dim(jnp.concatenate([t_pad, t_pad]), NZ - 1 - level, NZ, 0)
    far = {
        j: lax.ppermute(jnp.concatenate([x_pad, t_want[j]], axis=1), "z", ring(-j))
        for j in A_FAR + B_FAR
    }
    t_own = jnp.stack(
        [
            far[j][:, BLK:]
            if j in far
            else lax.ppermute(t_want[j], "z", ring(-j)) if j else t_want[0]
            for j in range(NZ)
        ]
    )
    t_oth = core_swap(t_own)
    a_parts = around(jnp.stack([far[j][:, :BLK] for j in A_FAR]), "x", "y")
    b_parts = around(jnp.stack([far[j][:, :BLK] for j in B_FAR]), "y", "x")
    x_own = xz[:, :PAD]
    x_up = lax.ppermute(x_own, "z", ring(-1))
    x_down = lax.ppermute(x_own, "z", ring(1))
    xs = (xz, x_up, x_down, *a_parts, *b_parts)

    z_all = xz.reshape(NZ, NC, PAD + QC, BLK)
    z_own = lax.dynamic_index_in_dim(z_all, core, 1, keepdims=False)[:, PAD:]
    z_oth = lax.dynamic_index_in_dim(z_all, 1 - core, 1, keepdims=False)[:, PAD:]
    z_here = jnp.stack([z_own, core_swap(z_oth)])
    ups, downs = [z_here], [z_here]
    for _ in range(3):
        ups.append(lax.ppermute(ups[-1], "z", ring(-1)))
        downs.append(lax.ppermute(downs[-1], "z", ring(1)))
    last_up = lax.ppermute(ups[-1][:1], "z", ring(-1))
    last_down = lax.ppermute(downs[-1][1:], "z", ring(1))
    z_pieces = (*ups, *downs[1:], last_up, last_down)

    h_msg = make_half(place, t_own, t_oth, xs)
    h_own = lax.all_to_all(h_msg, XY, split_axis=0, concat_axis=0, tiled=True)
    h_own = h_own.reshape(NV * PAD, HALF_M)
    h_oth = core_swap(h_own)

    b_own, b_send = make_main(place, h_own, h_oth, xs, z_pieces)
    b_sum = (b_own + core_swap(b_send).astype(F32)).astype(BF)
    b_all = lax.all_to_all(
        b_sum.reshape(NV, PAD, HALF_M), XY, split_axis=0, concat_axis=0, tiled=True
    )

    l_own, l_send = make_ladder(place, b_all, xs)
    l_recv = core_swap(l_send)
    other_part = lax.dynamic_index_in_dim(other_terms, level, 0, keepdims=False)
    other_part = jnp.pad(other_part, ((0, PAD - ROW), (0, 0)))
    other_part = lax.dynamic_slice_in_dim(other_part, core * HALF, HALF, 0)
    row_energy = lax.dynamic_slice_in_dim(virt_energy, lax.axis_index(XY) * ROW, ROW, 0)
    low_energy = jnp.pad(row_energy, (0, PAD - ROW), constant_values=1.0)
    low_energy = lax.dynamic_slice_in_dim(low_energy, core * HALF, HALF, 0)
    low_energy = (low_energy - lax.dynamic_index_in_dim(pair_energy, level, 0))[:, None]
    chunk = make_chunk(place, l_own, l_recv, other_part, virt_energy[None, :], low_energy)
    l_mine = lax.all_gather(chunk, "z", axis=0)
    l_rest = core_swap(l_mine)

    marks = jnp.concatenate([l_mine, l_rest])
    squares = jnp.sum(marks[:, 0, NVIR : NVIR + 3].astype(F32))
    total = jnp.broadcast_to(squares, (NV, 8, LANE))
    totals = lax.all_to_all(total, XY, split_axis=0, concat_axis=0, tiled=True)
    other_rows = jnp.transpose(other_terms, (1, 0, 2))
    residual = jnp.transpose(make_final(place, l_mine, l_rest, other_rows), (1, 0, 2))
    count = PAIRS * NVIR * NVIR
    update_rms = jnp.sqrt(jnp.sum(totals[:, 0, 0]) / count + epsilon)
    return residual, update_rms


def solution(mesh):
    torus = Mesh(mesh.devices.reshape(NX, NY, NZ, NC), AXES)
    return jax.shard_map(
        shards,
        mesh=torus,
        in_specs=(
            P(None, XY, RANK),
            P(XY, RANK),
            P(XY, RANK),
            P(None, XY, None),
            P(),
            P(),
        ),
        out_specs=(P(None, XY, None), P()),
        check_vma=False,
    )
```
